128 devices in a mesh: gx: 2 (over core), gy: 64 (over z, y, x).
Axes of the slice: x: 4, y: 4, z: 4, core: 2. Of those that a mesh axis runs over, the one named last changes fastest.
Arguments:
- right_side: float32 [128, 16384], P('gx', 'gy'), may hold values from -34 to 34, as said below
- initial: float32 [128, 16384], P('gx', 'gy'), may hold values from -0.6 to 0.6
- reaction: float32 [128, 16384], P('gx', 'gy'), may hold values from 0.05 to 0.5
- velocity_x: float32 [128, 16384], P('gx', 'gy'), may hold values from -1 to 1
- velocity_y: float32 [128, 16384], P('gx', 'gy'), may hold values from -1 to 1
Outputs:
- solution: float32 [128, 16384], P('gx', 'gy')
- residual: float32 [128, 16384], P('gx', 'gy')
The draws below stay inside these ranges and needn't reach their ends.
Inputs may be any that keep to these rules, and one draw needn't show every extreme that they name: right_side is noise bounded by 4 in size times an envelope 0.5 + 8 g, where g is a periodic Gaussian bump of one device block's width along each dimension centred at a drawn position, so its entries lie within -34 and 34.
All inputs are finite; a program needn't handle non-finite values.
Results may differ from the reference program's by a relative error of at most 0.0075.
Values sent between devices are 32-bit elements.
A program may use at most 64 MiB of HBM per device.

```python
import math
import jax
import jax.numpy as jnp
from jax import lax

CX = 64
CY = 256
RESTART = 15
NX = 128
NY = 16384


def draw_right_side(key, part):
    noise_key = jax.random.fold_in(key, 11)
    centre_key = jax.random.fold_in(key, 12)
    noise = jnp.clip(jax.random.normal(noise_key, (NX, NY), jnp.float32), -4.0, 4.0)
    centre = jax.random.uniform(centre_key, (2,), jnp.float32)
    along_x = jnp.mod(jnp.arange(NX, dtype=jnp.float32) - centre[0] * NX, NX)
    along_y = jnp.mod(jnp.arange(NY, dtype=jnp.float32) - centre[1] * NY, NY)
    gap_x = jnp.minimum(along_x, NX - along_x) / CX
    gap_y = jnp.minimum(along_y, NY - along_y) / CY
    bump = jnp.exp(-0.5 * (gap_x[:, None] * gap_x[:, None] + gap_y[None, :] * gap_y[None, :]))
    return noise * (0.5 + 8.0 * bump)


def block_levels(key, dims, pieces, smallest, top_value):
    def one(dim, parts):
        draws = jax.random.uniform(jax.random.fold_in(jax.random.fold_in(key, 6), dim), (parts,), jnp.float32, smallest / len(pieces), top_value / len(pieces))
        return jnp.repeat(jnp.exp(draws), dims[dim] // parts).reshape((-1,) + (1,) * (len(dims) - dim - 1))

    gain = one(*pieces[0])
    for cut in pieces[1:]:
        gain = gain * one(*cut)
    return gain


def scatter_about(stream_key, extent, deviation, limit, split=(), held_as=jnp.bfloat16):
    loudness = block_levels(stream_key, extent, split, -0.22, 0.18) if split else 1.0
    drawn = jax.random.normal(stream_key, extent, jnp.float32) * deviation * loudness
    return jnp.minimum(jnp.maximum(drawn, -limit), limit).astype(held_as)


def setup_inputs(seed: int = 0) -> dict:
    arg_keys = jax.random.split(jax.random.key(seed), 6)
    return {
        "right_side": draw_right_side(jax.random.fold_in(arg_keys[5], 71), 0),
        "initial": scatter_about(arg_keys[1], (NX, NY), 0.1, 0.6, ((0, 2), (1, 64)), jnp.float32),
        "reaction": jnp.clip(jnp.exp(math.log(0.5) - 2.3025851 * jax.random.uniform(arg_keys[2], (NX, NY), jnp.float32) ** block_levels(arg_keys[2], (NX, NY), ((0, 2), (1, 64)), -0.2, 0.2)), 0.05, 0.5),
        "velocity_x": jnp.clip(jax.random.uniform(arg_keys[3], (NX, NY), jnp.float32, -1.0, 1.0) * block_levels(arg_keys[3], (NX, NY), ((0, 2), (1, 64)), -0.4, 0.0), -1.0, 1.0),
        "velocity_y": jnp.clip(jax.random.uniform(arg_keys[4], (NX, NY), jnp.float32, -1.0, 1.0) * block_levels(arg_keys[4], (NX, NY), ((0, 2), (1, 64)), -0.4, 0.0), -1.0, 1.0),
    }


def moved(field, offset, dimension):
    return jnp.roll(field, -offset, dimension)

def first_diff(field, dimension):
    outer = moved(field, -2, dimension) - moved(field, 2, dimension)
    inner = moved(field, 1, dimension) - moved(field, -1, dimension)
    return (outer + 8.0 * inner) / 12.0

def second_diff(field, dimension):
    inner = moved(field, 1, dimension) + moved(field, -1, dimension)
    outer = moved(field, 2, dimension) + moved(field, -2, dimension)
    return (16.0 * inner - outer - 30.0 * field) / 12.0

def operate(field, reaction, velocity_x, velocity_y):
    diffusion = second_diff(field, 0) + second_diff(field, 1)
    advect_x = 0.5 * (velocity_x * first_diff(field, 0) + first_diff(velocity_x * field, 0))
    advect_y = 0.5 * (velocity_y * first_diff(field, 1) + first_diff(velocity_y * field, 1))
    return reaction * field - diffusion + advect_x + advect_y

def least_squares(hessenberg, beta):
    columns_total = hessenberg.shape[1]
    target = jnp.where(jnp.arange(columns_total + 1) == 0, beta, 0.0)

    def rotate(column, carried):
        upper, target = carried
        top_row = upper[column]
        next_row = upper[column + 1]
        diagonal_entry = top_row[column]
        below_entry = next_row[column]
        radius = jnp.sqrt(diagonal_entry * diagonal_entry + below_entry * below_entry)
        cosine = diagonal_entry / radius
        sine_value = below_entry / radius
        upper = upper.at[column].set(cosine * top_row + sine_value * next_row)
        upper = upper.at[column + 1].set(cosine * next_row - sine_value * top_row)
        upper_value = target[column]
        lower_value = target[column + 1]
        target = target.at[column].set(cosine * upper_value + sine_value * lower_value)
        target = target.at[column + 1].set(cosine * lower_value - sine_value * upper_value)
        return (upper, target)
    upper, target = lax.fori_loop(0, columns_total, rotate, (hessenberg, target))

    def substitute(count, weights):
        row_index = columns_total - 1 - count
        known = jnp.sum(upper[row_index] * weights)
        return weights.at[row_index].set((target[row_index] - known) / upper[row_index, row_index])
    return lax.fori_loop(0, columns_total, substitute, jnp.zeros((columns_total,), jnp.float32))

def reference(right_side, initial, reaction, velocity_x, velocity_y):

    def operator_on(field):
        return operate(field, reaction, velocity_x, velocity_y)
    start_residual = right_side - operator_on(initial)
    beta = jnp.sqrt(jnp.sum(start_residual * start_residual))
    basis = [start_residual / beta]
    hessenberg = jnp.zeros((RESTART + 1, RESTART), jnp.float32)
    for column in range(RESTART):
        applied = operator_on(basis[column])
        projection = jnp.stack([jnp.sum(vector * applied) for vector in basis])
        correction = jnp.zeros_like(applied)
        for position, vector in enumerate(basis):
            correction = correction + projection[position] * vector
        applied = applied - correction
        length = jnp.sqrt(jnp.sum(applied * applied))
        hessenberg = hessenberg.at[:column + 1, column].set(projection)
        hessenberg = hessenberg.at[column + 1, column].set(length)
        basis.append(applied / length)
    weights = least_squares(hessenberg, beta)
    solution = initial
    for position in range(RESTART):
        solution = solution + weights[position] * basis[position]
    residual = right_side - operator_on(solution)
    return (solution, residual)
```

```python
import functools

import jax
import jax.numpy as jnp
import numpy as np
from jax import lax
from jax.experimental import pallas as pl
from jax.experimental.pallas import tpu as pltpu
from jax.sharding import PartitionSpec as P

MESH = pl.DeviceIdType.MESH
STEPS = 15
CHUNK = 32
F32 = jnp.float32


def recurrence():
    count = 128
    angle = (np.arange(count) + 0.5) * np.pi / count
    one = (30.0 - 32.0 * np.cos(angle) + 2.0 * np.cos(2.0 * angle)) / 12.0
    values = (0.2 + one[:, None] + one[None, :]).ravel()
    weight = values * values
    scale = 4.0 / (values.max() - values.min())
    values = values * scale
    before, now, norm_before = np.zeros_like(values), np.ones_like(values), 1.0
    centres, links = [], []
    for k in range(STEPS):
        norm = (weight * now * now).sum()
        centre = (weight * values * now * now).sum() / norm
        link = norm / norm_before if k else 0.0
        centres.append(float(centre))
        links.append(float(link))
        before, now, norm_before = now, (values - centre) * now - link * before, norm
    return float(scale), centres, links


SCALE, CENTRES, LINKS = recurrence()

BLOCKS = [(i, j) for i in range(4) for j in range(i, 4)]
SLOT = {}
for number, (bi, bj) in enumerate(BLOCKS):
    for a in range(4):
        for b in range(4):
            SLOT.setdefault((4 * bi + a, 4 * bj + b), number * 16 + a * 4 + b)


def lanes(shape):
    return lax.broadcasted_iota(jnp.int32, shape, 1)


def kernel(gy, *refs):
    ins, outs = refs[:5], refs[5:7]
    (buf, send, halo, speed, coef, field, image, acc, msg, every, spread, done, table,
     in_sem, part_sem, edge_sem, halo_sem, sum_sem, out_sem, far_sem) = refs[7:]
    c = lax.axis_index("gx")
    g = lax.axis_index("gy")
    n = 2 * gy
    me = c * gy + g
    mine = pl.multiple_of(c * 64, 64)
    theirs = pl.multiple_of((1 - c) * 64, 64)
    my_cols = pl.multiple_of(c * 128, 128)

    loads = [pltpu.make_async_copy(ins[q], buf.at[q, pl.ds(mine, 64)], in_sem.at[q]) for q in range(5)]
    for load in loads:
        load.start()

    barrier = pltpu.get_barrier_semaphore()

    def greet(step, carry):
        to = lax.rem(me + step, n)
        pl.semaphore_signal(barrier, inc=1, device_id=(to // gy, lax.rem(to, gy)), device_id_type=MESH)
        return carry

    lax.fori_loop(1, n, greet, 0)

    for k in range(STEPS):
        table[0, k] = CENTRES[k]
        table[1, k] = LINKS[k]
    for load in loads:
        load.wait()

    lane64 = lanes((64, 128))
    lane16 = lanes((16, 128))
    for way in range(2):
        tile, first = (1, 96) if way == 0 else (0, 0)
        packed = None
        for q in range(4):
            at = 32 * (q if way == 0 else (q + 1) % 4)
            piece = buf[q, pl.ds(mine, 64), pl.ds(128 * tile, 128)]
            shift = (at - first) % 128
            piece = pltpu.roll(piece, shift, 1) if shift else piece
            packed = piece if packed is None else jnp.where((lane64 >= at) & (lane64 < at + 32), piece, packed)
        send[way, pl.ds(0, 64)] = packed
        packed = None
        for q in range(4):
            at = 32 * (q if way == 0 else (q + 1) % 4)
            piece = buf[4, pl.ds(pl.multiple_of(mine + 16 * q, 16), 16), pl.ds(128 * tile, 128)]
            shift = (at - first) % 128
            piece = pltpu.roll(piece, shift, 1) if shift else piece
            packed = piece if packed is None else jnp.where((lane16 >= at) & (lane16 < at + 32), piece, packed)
        send[way, pl.ds(64, 16)] = packed

    pl.semaphore_wait(barrier, n - 1)

    edges = []
    for way, (core, chip) in enumerate(((0, lax.rem(g + 1, gy)), (1, lax.rem(g + gy - 1, gy)))):
        edge = pltpu.make_async_remote_copy(
            send.at[way], halo.at[c], edge_sem.at[way], halo_sem.at[c], device_id=(core, chip), device_id_type=MESH
        )
        edge.start()
        edges.append(edge)
    part = pltpu.make_async_remote_copy(
        buf.at[:, pl.ds(mine, 64)], buf.at[:, pl.ds(mine, 64)], part_sem.at[0], part_sem.at[1],
        device_id=(1 - c, g), device_id_type=MESH,
    )
    part.start()
    part.wait()
    for side in range(2):
        pltpu.make_async_copy(halo.at[side], halo.at[side], halo_sem.at[side]).wait()

    def gather(q, rows):
        side = rows // 64
        low = rows % 64
        lane = lanes((CHUNK, 128))
        own = pltpu.roll(buf[q, pl.ds(rows, CHUNK), pl.ds(my_cols, 128)], 32, 1)
        near = pltpu.roll(buf[q, pl.ds(rows, CHUNK), pl.ds(pl.multiple_of(128 - my_cols, 128), 128)], 32, 1)
        if q < 4:
            far = halo[side, pl.ds(low, CHUNK)]
            far = pltpu.roll(far, 128 - 32 * q, 1) if q else far
        else:
            pieces = []
            for k in range(low // 16, low // 16 + CHUNK // 16):
                piece = halo[side, pl.ds(64, 16)]
                pieces.append(pltpu.roll(piece, 128 - 32 * k, 1) if k else piece)
            far = jnp.concatenate(pieces, axis=0)
        edge = jnp.where((lane < 32).astype(jnp.int32) == (1 - c), far, near)
        return jnp.where(lane < 32, edge, own), jnp.where((lane >= 32) & (lane < 64), edge, own)

    def put(ref, at, rows, value):
        ref[at + (pl.ds(8 + rows, CHUNK),)] = value
        if rows == 0:
            ref[at + (pl.ds(136, 8),)] = value[:8]
        if rows == 128 - CHUNK:
            ref[at + (pl.ds(0, 8),)] = value[CHUNK - 8 :]

    ROWS = range(0, 128, CHUNK)
    for rows in ROWS:
        for tile, value in enumerate(gather(1, rows)):
            put(field, (0, tile), rows, value)
        for tile, value in enumerate(gather(3, rows)):
            put(speed, (tile,), rows, value)
    for rows in ROWS:
        here = pl.ds(rows, CHUNK)
        reaction = gather(2, rows)
        along = gather(4, rows)
        for tile in range(2):
            coef[0, tile, here] = SCALE * (reaction[tile] + 5.0)
            vx = speed[tile, pl.ds(8 + rows, CHUNK)]
            for number, (offset, flat, slope) in enumerate(STENCIL):
                other = speed[tile, pl.ds(8 + rows + offset, CHUNK)]
                coef[1 + number, tile, here] = flat + slope * (vx + other)
            vy = along[tile]
            for number, (offset, flat, slope) in enumerate(STENCIL):
                other = pltpu.roll(vy, (-offset) % 128, 1)
                coef[5 + number, tile, here] = flat + slope * (vy + other)

    def operate(slot, tile, rows):
        here = pl.ds(rows, CHUNK)
        centre = field[slot, tile, pl.ds(8 + rows, CHUNK)]
        total = coef[0, tile, here] * centre
        for number, (offset, _, _) in enumerate(STENCIL):
            total = total + coef[1 + number, tile, here] * field[slot, tile, pl.ds(8 + rows + offset, CHUNK)]
        for number, (offset, _, _) in enumerate(STENCIL):
            total = total + coef[5 + number, tile, here] * pltpu.roll(centre, (-offset) % 128, 1)
        return centre, total

    def core(lane, first, second):
        return jnp.where((lane >= 32) & (lane < 96), first, second)

    lane = lanes((CHUNK, 128))
    for rows in ROWS:
        right = gather(0, rows)
        start = []
        for tile in range(2):
            _, total = operate(0, tile, rows)
            value = right[tile] - (1.0 / SCALE) * total
            put(field, (1, tile), rows, value)
            start.append(value)
        image[STEPS, pl.ds(rows, CHUNK)] = core(lane, *start)

    def step(k, carry):
        centre_k = table[0, k]
        link_k = table[1, k]
        for rows in ROWS:
            both = []
            for tile in range(2):
                now, total = operate(k + 1, tile, rows)
                before = field[k, tile, pl.ds(8 + rows, CHUNK)]
                put(field, (k + 2, tile), rows, total - centre_k * now - link_k * before)
                both.append(total)
            image[k, pl.ds(rows, CHUNK)] = core(lane, *both)
        return carry

    lax.fori_loop(0, STEPS, step, 0)

    for number, (bi, bj) in enumerate(BLOCKS):

        def products(row, sums, bi=bi, bj=bj):
            at = pl.ds(pl.multiple_of(row * 8, 8), 8)
            left = [image[4 * bi + a, at] for a in range(4)]
            right = left if bi == bj else [image[4 * bj + b, at] for b in range(4)]
            return tuple(sums[4 * a + b] + left[a] * right[b] for a in range(4) for b in range(4))

        sums = lax.fori_loop(0, 16, products, (jnp.zeros((8, 128), F32),) * 16)
        for a in range(16):
            acc[number * 16 + a] = sums[a]

    totals = jnp.sum(jnp.sum(acc[...], axis=1), axis=1, keepdims=True)
    wide = jnp.broadcast_to(totals[:128], (128, 128))
    pick = lax.broadcasted_iota(jnp.int32, (128, 128), 0) == lanes((128, 128))
    msg[pl.ds(0, 1)] = jnp.sum(jnp.where(pick, wide, 0.0), axis=0, keepdims=True)
    wide = jnp.broadcast_to(totals[128:], (32, 128))
    msg[pl.ds(1, 1)] = jnp.sum(jnp.where(pick[:32], wide, 0.0), axis=0, keepdims=True)

    def tell(step, carry):
        to = lax.rem(me + step, n)
        pltpu.make_async_remote_copy(
            msg, every.at[me], sum_sem.at[0], sum_sem.at[1],
            device_id=(to // gy, lax.rem(to, gy)), device_id_type=MESH,
        ).start()
        return carry

    lax.fori_loop(1, n, tell, 0)
    every[me] = msg[...]
    others = every.at[pl.ds(0, n - 1)]
    pltpu.make_async_copy(others, others, sum_sem.at[1]).wait()
    total = jnp.sum(every[...], axis=0)

    wide = jnp.where(pick, jnp.broadcast_to(total[0:1], (128, 128)), 0.0)
    spread[pl.ds(0, 128)] = jnp.broadcast_to(jnp.sum(wide, axis=1, keepdims=True), (128, 128))
    wide = jnp.where(pick[:32], jnp.broadcast_to(total[1:2], (32, 128)), 0.0)
    spread[pl.ds(128, 32)] = jnp.broadcast_to(jnp.sum(wide, axis=1, keepdims=True), (32, 128))

    def entry(i, j):
        at = SLOT[(min(i, j), max(i, j))]
        return jnp.broadcast_to(spread[at : at + 1], (8, 128))

    gram = [[entry(i, j) for j in range(i + 1)] for i in range(STEPS)]
    goal = [entry(i, STEPS) for i in range(STEPS)]
    inverse = []
    for k in range(STEPS):
        inverse.append(1.0 / gram[k][k])
        for i in range(k + 1, STEPS):
            ratio = gram[i][k] * inverse[k]
            for j in range(k + 1, i + 1):
                gram[i][j] = gram[i][j] - ratio * gram[j][k]
            goal[i] = goal[i] - ratio * goal[k]
    weights = [None] * STEPS
    for k in reversed(range(STEPS)):
        value = goal[k]
        for i in range(k + 1, STEPS):
            value = value - gram[i][k] * weights[i]
        weights[k] = value * inverse[k]

    lane8 = lanes((8, 128))

    def finish(row, carry):
        at = pl.ds(pl.multiple_of(row * 8, 8), 8)
        inner = pl.ds(pl.multiple_of(row * 8 + 8, 8), 8)
        leftover = image[STEPS, at]
        change = jnp.zeros((8, 128), F32)
        for k in range(STEPS):
            leftover = leftover - weights[k] * image[k, at]
            change = change + weights[k] * core(lane8, field[k + 1, 0, inner], field[k + 1, 1, inner])
        start = core(lane8, field[0, 0, inner], field[0, 1, inner])
        done[0, at] = pltpu.roll(start + SCALE * change, 96, 1)
        done[1, at] = pltpu.roll(leftover, 96, 1)
        return carry

    lax.fori_loop(0, 16, finish, 0)

    ends = []
    for o in range(2):
        away = pltpu.make_async_remote_copy(
            done.at[o, pl.ds(theirs, 64)], outs[o].at[:, pl.ds(my_cols, 128)], far_sem.at[0, o], far_sem.at[1, o],
            device_id=(1 - c, g), device_id_type=MESH,
        )
        away.start()
        home = pltpu.make_async_copy(done.at[o, pl.ds(mine, 64)], outs[o].at[:, pl.ds(my_cols, 128)], out_sem.at[o])
        home.start()
        ends += [away, home]
    for end in ends:
        end.wait()
    for edge in edges:
        edge.wait_send()
    pltpu.make_async_copy(others, others, sum_sem.at[0]).wait()


STENCIL = [
    (-2, SCALE / 12.0, SCALE / 24.0),
    (-1, -SCALE * 16.0 / 12.0, -SCALE * 8.0 / 24.0),
    (1, -SCALE * 16.0 / 12.0, SCALE * 8.0 / 24.0),
    (2, SCALE / 12.0, -SCALE / 24.0),
]


def solution(mesh):
    gy = mesh.shape["gy"]
    n = 2 * gy
    anywhere = pl.BlockSpec(memory_space=pl.ANY)

    def per_device(*blocks):
        return pl.pallas_call(
            functools.partial(kernel, gy),
            out_shape=[jax.ShapeDtypeStruct((64, 256), F32)] * 2,
            in_specs=[anywhere] * 5,
            out_specs=[anywhere] * 2,
            scratch_shapes=[
                pltpu.VMEM((5, 128, 256), F32),
                pltpu.VMEM((2, 80, 128), F32),
                pltpu.VMEM((2, 80, 128), F32),
                pltpu.VMEM((2, 144, 128), F32),
                pltpu.VMEM((9, 2, 128, 128), F32),
                pltpu.VMEM((STEPS + 2, 2, 144, 128), F32),
                pltpu.VMEM((STEPS + 1, 128, 128), F32),
                pltpu.VMEM((160, 8, 128), F32),
                pltpu.VMEM((2, 128), F32),
                pltpu.VMEM((n, 2, 128), F32),
                pltpu.VMEM((160, 128), F32),
                pltpu.VMEM((2, 128, 128), F32),
                pltpu.SMEM((2, 16), F32),
                pltpu.SemaphoreType.DMA((5,)),
                pltpu.SemaphoreType.DMA((2,)),
                pltpu.SemaphoreType.DMA((2,)),
                pltpu.SemaphoreType.DMA((2,)),
                pltpu.SemaphoreType.DMA((2,)),
                pltpu.SemaphoreType.DMA((2,)),
                pltpu.SemaphoreType.DMA((2, 2)),
            ],
            compiler_params=pltpu.CompilerParams(collective_id=0, has_side_effects=True),
        )(*blocks)

    placed = P("gx", "gy")
    return jax.shard_map(
        per_device, mesh=mesh, in_specs=(placed,) * 5, out_specs=(placed, placed), check_vma=False
    )
```

```python
import functools

import jax
import jax.numpy as jnp
import numpy as np
from jax import lax
from jax.experimental import pallas as pl
from jax.experimental.pallas import tpu as pltpu
from jax.sharding import PartitionSpec as P

MESH = pl.DeviceIdType.MESH
STEPS = 15
CHUNK = 32
F32 = jnp.float32


def recurrence():
    count = 128
    angle = (np.arange(count) + 0.5) * np.pi / count
    one = (30.0 - 32.0 * np.cos(angle) + 2.0 * np.cos(2.0 * angle)) / 12.0
    values = (0.2 + one[:, None] + one[None, :]).ravel()
    weight = values * values
    scale = 4.0 / (values.max() - values.min())
    values = values * scale
    before, now, norm_before = np.zeros_like(values), np.ones_like(values), 1.0
    centres, links = [], []
    for k in range(STEPS):
        norm = (weight * now * now).sum()
        centre = (weight * values * now * now).sum() / norm
        link = norm / norm_before if k else 0.0
        centres.append(float(centre))
        links.append(float(link))
        before, now, norm_before = now, (values - centre) * now - link * before, norm
    return float(scale), centres, links


SCALE, CENTRES, LINKS = recurrence()

BLOCKS = [(i, j) for i in range(4) for j in range(i, 4)]
SLOT = {}
for number, (bi, bj) in enumerate(BLOCKS):
    for a in range(4):
        for b in range(4):
            SLOT.setdefault((4 * bi + a, 4 * bj + b), number * 16 + a * 4 + b)


def lanes(shape):
    return lax.broadcasted_iota(jnp.int32, shape, 1)


def kernel(gy, *refs):
    ins, outs = refs[:5], refs[5:7]
    (buf, send, halo, speed, coef, field, image, acc, msg, every, spread, done, table,
     in_sem, part_sem, edge_sem, halo_sem, sum_sem, out_sem, far_sem, meet) = refs[7:]
    c = lax.axis_index("gx")
    g = lax.axis_index("gy")
    n = 2 * gy
    me = c * gy + g
    mine = pl.multiple_of(c * 64, 64)
    theirs = pl.multiple_of((1 - c) * 64, 64)
    my_cols = pl.multiple_of(c * 128, 128)

    loads = [pltpu.make_async_copy(ins[q], buf.at[q, pl.ds(mine, 64)], in_sem.at[q]) for q in range(5)]
    for load in loads:
        load.start()

    sizes = (4, 4, 4) if gy == 64 else (1, 2, gy // 2)
    strides = (sizes[1] * sizes[2], sizes[2], 1)
    around = [
        [lax.rem(lax.rem(g // stride, size) + k, size) * stride for k in range(size)]
        for stride, size in zip(strides, sizes)
    ]
    ahead, behind = lax.rem(g + 1, gy), lax.rem(g + gy - 1, gy)

    def line(d):
        rest = g - around[d][0]
        return [(c, rest + around[d][k]) for k in sorted(range(1, sizes[d]), key=lambda k: k != sizes[d] // 2)]

    def signal(sem, to):
        pl.semaphore_signal(sem, inc=1, device_id=to, device_id_type=MESH)

    barrier = pltpu.get_barrier_semaphore()
    sender = jnp.where(c == 0, behind, ahead)
    greeted = [(0, sender), (1, sender)] + line(0) + line(1) + line(2) + [(1 - c, g)]
    for to in greeted:
        signal(barrier, to)

    for k in range(STEPS):
        table[0, k] = CENTRES[k]
        table[1, k] = LINKS[k]
    for load in loads:
        load.wait()

    lane64 = lanes((64, 128))
    lane16 = lanes((16, 128))
    for way in range(2):
        tile, first = (1, 96) if way == 0 else (0, 0)
        packed = None
        for q in range(4):
            at = 32 * (q if way == 0 else (q + 1) % 4)
            piece = buf[q, pl.ds(mine, 64), pl.ds(128 * tile, 128)]
            shift = (at - first) % 128
            piece = pltpu.roll(piece, shift, 1) if shift else piece
            packed = piece if packed is None else jnp.where((lane64 >= at) & (lane64 < at + 32), piece, packed)
        send[way, pl.ds(0, 64)] = packed
        packed = None
        for q in range(4):
            at = 32 * (q if way == 0 else (q + 1) % 4)
            piece = buf[4, pl.ds(pl.multiple_of(mine + 16 * q, 16), 16), pl.ds(128 * tile, 128)]
            shift = (at - first) % 128
            piece = pltpu.roll(piece, shift, 1) if shift else piece
            packed = piece if packed is None else jnp.where((lane16 >= at) & (lane16 < at + 32), piece, packed)
        send[way, pl.ds(64, 16)] = packed

    pl.semaphore_wait(barrier, len(greeted))

    edges = []
    for way, (core, chip) in enumerate(((0, ahead), (1, behind))):
        edge = pltpu.make_async_remote_copy(
            send.at[way], halo.at[c], edge_sem.at[way], halo_sem.at[c], device_id=(core, chip), device_id_type=MESH
        )
        edge.start()
        edges.append(edge)
    part = pltpu.make_async_remote_copy(
        buf.at[:, pl.ds(mine, 64)], buf.at[:, pl.ds(mine, 64)], part_sem.at[0], part_sem.at[1],
        device_id=(1 - c, g), device_id_type=MESH,
    )
    part.start()
    for to in line(2):
        signal(meet.at[0], to)
    part.wait()
    for side in range(2):
        pltpu.make_async_copy(halo.at[side], halo.at[side], halo_sem.at[side]).wait()

    pl.semaphore_wait(meet.at[0], sizes[2] - 1)
    for to in line(1):
        signal(meet.at[1], to)
    def gather(q, rows):
        side = rows // 64
        low = rows % 64
        lane = lanes((CHUNK, 128))
        own = pltpu.roll(buf[q, pl.ds(rows, CHUNK), pl.ds(my_cols, 128)], 32, 1)
        near = pltpu.roll(buf[q, pl.ds(rows, CHUNK), pl.ds(pl.multiple_of(128 - my_cols, 128), 128)], 32, 1)
        if q < 4:
            far = halo[side, pl.ds(low, CHUNK)]
            far = pltpu.roll(far, 128 - 32 * q, 1) if q else far
        else:
            pieces = []
            for k in range(low // 16, low // 16 + CHUNK // 16):
                piece = halo[side, pl.ds(64, 16)]
                pieces.append(pltpu.roll(piece, 128 - 32 * k, 1) if k else piece)
            far = jnp.concatenate(pieces, axis=0)
        edge = jnp.where((lane < 32).astype(jnp.int32) == (1 - c), far, near)
        return jnp.where(lane < 32, edge, own), jnp.where((lane >= 32) & (lane < 64), edge, own)

    def put(ref, at, rows, value):
        ref[at + (pl.ds(8 + rows, CHUNK),)] = value
        if rows == 0:
            ref[at + (pl.ds(136, 8),)] = value[:8]
        if rows == 128 - CHUNK:
            ref[at + (pl.ds(0, 8),)] = value[CHUNK - 8 :]

    ROWS = range(0, 128, CHUNK)
    for rows in ROWS:
        for tile, value in enumerate(gather(1, rows)):
            put(field, (0, tile), rows, value)
        for tile, value in enumerate(gather(3, rows)):
            put(speed, (tile,), rows, value)
    for rows in ROWS:
        here = pl.ds(rows, CHUNK)
        reaction = gather(2, rows)
        along = gather(4, rows)
        for tile in range(2):
            coef[0, tile, here] = SCALE * (reaction[tile] + 5.0)
            vx = speed[tile, pl.ds(8 + rows, CHUNK)]
            for number, (offset, flat, slope) in enumerate(STENCIL):
                other = speed[tile, pl.ds(8 + rows + offset, CHUNK)]
                coef[1 + number, tile, here] = flat + slope * (vx + other)
            vy = along[tile]
            for number, (offset, flat, slope) in enumerate(STENCIL):
                other = pltpu.roll(vy, (-offset) % 128, 1)
                coef[5 + number, tile, here] = flat + slope * (vy + other)

    def operate(slot, tile, rows):
        here = pl.ds(rows, CHUNK)
        centre = field[slot, tile, pl.ds(8 + rows, CHUNK)]
        total = coef[0, tile, here] * centre
        for number, (offset, _, _) in enumerate(STENCIL):
            total = total + coef[1 + number, tile, here] * field[slot, tile, pl.ds(8 + rows + offset, CHUNK)]
        for number, (offset, _, _) in enumerate(STENCIL):
            total = total + coef[5 + number, tile, here] * pltpu.roll(centre, (-offset) % 128, 1)
        return centre, total

    def core(lane, first, second):
        return jnp.where((lane >= 32) & (lane < 96), first, second)

    lane = lanes((CHUNK, 128))
    for rows in ROWS:
        right = gather(0, rows)
        start = []
        for tile in range(2):
            _, total = operate(0, tile, rows)
            value = right[tile] - (1.0 / SCALE) * total
            put(field, (1, tile), rows, value)
            start.append(value)
        image[STEPS, pl.ds(rows, CHUNK)] = core(lane, *start)

    pl.semaphore_wait(meet.at[1], sizes[1] - 1)
    for to in line(0):
        signal(meet.at[2], to)
    def step(k, carry):
        centre_k = table[0, k]
        link_k = table[1, k]
        for rows in ROWS:
            both = []
            for tile in range(2):
                now, total = operate(k + 1, tile, rows)
                before = field[k, tile, pl.ds(8 + rows, CHUNK)]
                put(field, (k + 2, tile), rows, total - centre_k * now - link_k * before)
                both.append(total)
            image[k, pl.ds(rows, CHUNK)] = core(lane, *both)
        return carry

    lax.fori_loop(0, STEPS, step, 0)

    for number, (bi, bj) in enumerate(BLOCKS):

        def products(row, sums, bi=bi, bj=bj):
            at = pl.ds(pl.multiple_of(row * 8, 8), 8)
            left = [image[4 * bi + a, at] for a in range(4)]
            right = left if bi == bj else [image[4 * bj + b, at] for b in range(4)]
            return tuple(sums[4 * a + b] + left[a] * right[b] for a in range(4) for b in range(4))

        sums = lax.fori_loop(0, 16, products, (jnp.zeros((8, 128), F32),) * 16)
        for a in range(16):
            acc[number * 16 + a] = sums[a]

    totals = jnp.sum(jnp.sum(acc[...], axis=1), axis=1, keepdims=True)
    wide = jnp.broadcast_to(totals[:128], (128, 128))
    pick = lax.broadcasted_iota(jnp.int32, (128, 128), 0) == lanes((128, 128))
    msg[pl.ds(0, 1)] = jnp.sum(jnp.where(pick, wide, 0.0), axis=0, keepdims=True)
    wide = jnp.broadcast_to(totals[128:], (32, 128))
    msg[pl.ds(1, 1)] = jnp.sum(jnp.where(pick[:32], wide, 0.0), axis=0, keepdims=True)

    pl.semaphore_wait(meet.at[2], sizes[0] - 1)

    def hops(way):
        return sum(min(k, size - k) for k, size in zip(way[:3], sizes)) + 0.5 * way[3]

    ways = [(z, y, x, w) for z in range(sizes[0]) for y in range(sizes[1]) for x in range(sizes[2]) for w in range(2)]
    for z, y, x, w in sorted(ways[1:], key=hops, reverse=True):
        pltpu.make_async_remote_copy(
            msg, every.at[me], sum_sem.at[0], sum_sem.at[1],
            device_id=(1 - c if w else c, around[0][z] + around[1][y] + around[2][x]), device_id_type=MESH,
        ).start()
    every[me] = msg[...]
    others = every.at[pl.ds(0, n - 1)]
    pltpu.make_async_copy(others, others, sum_sem.at[1]).wait()
    total = jnp.sum(every[...], axis=0)

    wide = jnp.where(pick, jnp.broadcast_to(total[0:1], (128, 128)), 0.0)
    spread[pl.ds(0, 128)] = jnp.broadcast_to(jnp.sum(wide, axis=1, keepdims=True), (128, 128))
    wide = jnp.where(pick[:32], jnp.broadcast_to(total[1:2], (32, 128)), 0.0)
    spread[pl.ds(128, 32)] = jnp.broadcast_to(jnp.sum(wide, axis=1, keepdims=True), (32, 128))

    def entry(i, j):
        at = SLOT[(min(i, j), max(i, j))]
        return jnp.broadcast_to(spread[at : at + 1], (8, 128))

    gram = [[entry(i, j) for j in range(i + 1)] for i in range(STEPS)]
    goal = [entry(i, STEPS) for i in range(STEPS)]
    inverse = []
    for k in range(STEPS):
        inverse.append(1.0 / gram[k][k])
        for i in range(k + 1, STEPS):
            ratio = gram[i][k] * inverse[k]
            for j in range(k + 1, i + 1):
                gram[i][j] = gram[i][j] - ratio * gram[j][k]
            goal[i] = goal[i] - ratio * goal[k]
    weights = [None] * STEPS
    for k in reversed(range(STEPS)):
        value = goal[k]
        for i in range(k + 1, STEPS):
            value = value - gram[i][k] * weights[i]
        weights[k] = value * inverse[k]

    lane8 = lanes((8, 128))

    def finish(row, carry):
        at = pl.ds(pl.multiple_of(row * 8, 8), 8)
        inner = pl.ds(pl.multiple_of(row * 8 + 8, 8), 8)
        leftover = image[STEPS, at]
        change = jnp.zeros((8, 128), F32)
        for k in range(STEPS):
            leftover = leftover - weights[k] * image[k, at]
            change = change + weights[k] * core(lane8, field[k + 1, 0, inner], field[k + 1, 1, inner])
        start = core(lane8, field[0, 0, inner], field[0, 1, inner])
        done[0, at] = pltpu.roll(start + SCALE * change, 96, 1)
        done[1, at] = pltpu.roll(leftover, 96, 1)
        return carry

    lax.fori_loop(0, 16, finish, 0)

    ends = []
    for o in range(2):
        away = pltpu.make_async_remote_copy(
            done.at[o, pl.ds(theirs, 64)], outs[o].at[:, pl.ds(my_cols, 128)], far_sem.at[0, o], far_sem.at[1, o],
            device_id=(1 - c, g), device_id_type=MESH,
        )
        away.start()
        home = pltpu.make_async_copy(done.at[o, pl.ds(mine, 64)], outs[o].at[:, pl.ds(my_cols, 128)], out_sem.at[o])
        home.start()
        ends += [away, home]
    for end in ends:
        end.wait()
    for edge in edges:
        edge.wait_send()
    pltpu.make_async_copy(others, others, sum_sem.at[0]).wait()


STENCIL = [
    (-2, SCALE / 12.0, SCALE / 24.0),
    (-1, -SCALE * 16.0 / 12.0, -SCALE * 8.0 / 24.0),
    (1, -SCALE * 16.0 / 12.0, SCALE * 8.0 / 24.0),
    (2, SCALE / 12.0, -SCALE / 24.0),
]


def solution(mesh):
    gy = mesh.shape["gy"]
    n = 2 * gy
    anywhere = pl.BlockSpec(memory_space=pl.ANY)

    def per_device(*blocks):
        return pl.pallas_call(
            functools.partial(kernel, gy),
            out_shape=[jax.ShapeDtypeStruct((64, 256), F32)] * 2,
            in_specs=[anywhere] * 5,
            out_specs=[anywhere] * 2,
            scratch_shapes=[
                pltpu.VMEM((5, 128, 256), F32),
                pltpu.VMEM((2, 80, 128), F32),
                pltpu.VMEM((2, 80, 128), F32),
                pltpu.VMEM((2, 144, 128), F32),
                pltpu.VMEM((9, 2, 128, 128), F32),
                pltpu.VMEM((STEPS + 2, 2, 144, 128), F32),
                pltpu.VMEM((STEPS + 1, 128, 128), F32),
                pltpu.VMEM((160, 8, 128), F32),
                pltpu.VMEM((2, 128), F32),
                pltpu.VMEM((n, 2, 128), F32),
                pltpu.VMEM((160, 128), F32),
                pltpu.VMEM((2, 128, 128), F32),
                pltpu.SMEM((2, 16), F32),
                pltpu.SemaphoreType.DMA((5,)),
                pltpu.SemaphoreType.DMA((2,)),
                pltpu.SemaphoreType.DMA((2,)),
                pltpu.SemaphoreType.DMA((2,)),
                pltpu.SemaphoreType.DMA((2,)),
                pltpu.SemaphoreType.DMA((2,)),
                pltpu.SemaphoreType.DMA((2, 2)),
                pltpu.SemaphoreType.REGULAR((3,)),
            ],
            compiler_params=pltpu.CompilerParams(collective_id=0, has_side_effects=True),
        )(*blocks)

    placed = P("gx", "gy")
    return jax.shard_map(
        per_device, mesh=mesh, in_specs=(placed,) * 5, out_specs=(placed, placed), check_vma=False
    )
```

```python
import functools

import jax
import jax.numpy as jnp
import numpy as np
from jax import lax
from jax.experimental import pallas as pl
from jax.experimental.pallas import tpu as pltpu
from jax.sharding import PartitionSpec as P

MESH = pl.DeviceIdType.MESH
STEPS = 15
CHUNK = 32
F32 = jnp.float32


def recurrence():
    count = 128
    angle = (np.arange(count) + 0.5) * np.pi / count
    one = (30.0 - 32.0 * np.cos(angle) + 2.0 * np.cos(2.0 * angle)) / 12.0
    values = (0.2 + one[:, None] + one[None, :]).ravel()
    weight = values * values
    scale = 4.0 / (values.max() - values.min())
    values = values * scale
    before, now, norm_before = np.zeros_like(values), np.ones_like(values), 1.0
    centres, links = [], []
    for k in range(STEPS):
        norm = (weight * now * now).sum()
        centre = (weight * values * now * now).sum() / norm
        link = norm / norm_before if k else 0.0
        centres.append(float(centre))
        links.append(float(link))
        before, now, norm_before = now, (values - centre) * now - link * before, norm
    return float(scale), centres, links


SCALE, CENTRES, LINKS = recurrence()

BLOCKS = [(i, j) for i in range(4) for j in range(i, 4)]
SLOT = {}
for number, (bi, bj) in enumerate(BLOCKS):
    for a in range(4):
        for b in range(4):
            SLOT.setdefault((4 * bi + a, 4 * bj + b), number * 16 + a * 4 + b)


def lanes(shape):
    return lax.broadcasted_iota(jnp.int32, shape, 1)


def kernel(gy, *refs):
    ins, outs = refs[:5], refs[5:7]
    (buf, send, halo, plain, edge, speed, coef, field, image, acc, msg, every, spread, done, table,
     in_sem, part_sem, edge_sem, halo_sem, sum_sem, far_sem, meet) = refs[7:]
    c = lax.axis_index("gx")
    g = lax.axis_index("gy")
    n = 2 * gy
    me = c * gy + g
    mine = pl.multiple_of(c * 64, 64)
    theirs = pl.multiple_of((1 - c) * 64, 64)
    my_cols = pl.multiple_of(c * 128, 128)

    loads = [pltpu.make_async_copy(ins[q], buf.at[q, pl.ds(mine, 64)], in_sem.at[q]) for q in range(5)]
    for load in loads:
        load.start()

    sizes = (4, 4, 4) if gy == 64 else (1, 2, gy // 2)
    strides = (sizes[1] * sizes[2], sizes[2], 1)
    around = [
        [lax.rem(lax.rem(g // stride, size) + k, size) * stride for k in range(size)]
        for stride, size in zip(strides, sizes)
    ]
    ahead, behind = lax.rem(g + 1, gy), lax.rem(g + gy - 1, gy)

    def line(d):
        rest = g - around[d][0]
        return [(c, rest + around[d][k]) for k in sorted(range(1, sizes[d]), key=lambda k: k != sizes[d] // 2)]

    def signal(sem, to):
        pl.semaphore_signal(sem, inc=1, device_id=to, device_id_type=MESH)

    barrier = pltpu.get_barrier_semaphore()
    sender = jnp.where(c == 0, behind, ahead)
    across = [(1 - c, chip) for _, chip in line(0)]
    greeted = [(0, sender), (1, sender)] + line(0) + across + line(1) + line(2) + [(1 - c, g)]
    for to in greeted:
        signal(barrier, to)

    for k in range(STEPS):
        table[0, k] = CENTRES[k]
        table[1, k] = LINKS[k]
    for load in loads:
        load.wait()

    lane64 = lanes((64, 128))
    lane16 = lanes((16, 128))
    for way in range(2):
        tile, first = (1, 96) if way == 0 else (0, 0)
        packed = None
        for q in range(4):
            at = 32 * (q if way == 0 else (q + 1) % 4)
            piece = buf[q, pl.ds(mine, 64), pl.ds(128 * tile, 128)]
            shift = (at - first) % 128
            piece = pltpu.roll(piece, shift, 1) if shift else piece
            packed = piece if packed is None else jnp.where((lane64 >= at) & (lane64 < at + 32), piece, packed)
        send[way, pl.ds(0, 64)] = packed
        packed = None
        for q in range(4):
            at = 32 * (q if way == 0 else (q + 1) % 4)
            piece = buf[4, pl.ds(pl.multiple_of(mine + 16 * q, 16), 16), pl.ds(128 * tile, 128)]
            shift = (at - first) % 128
            piece = pltpu.roll(piece, shift, 1) if shift else piece
            packed = piece if packed is None else jnp.where((lane16 >= at) & (lane16 < at + 32), piece, packed)
        send[way, pl.ds(64, 16)] = packed

    pl.semaphore_wait(barrier, len(greeted))

    edges = []
    for way, (core, chip) in enumerate(((0, ahead), (1, behind))):
        copy = pltpu.make_async_remote_copy(
            send.at[way], halo.at[c], edge_sem.at[way], halo_sem.at[c], device_id=(core, chip), device_id_type=MESH
        )
        copy.start()
        edges.append(copy)
    part = pltpu.make_async_remote_copy(
        buf.at[:, pl.ds(mine, 64)], buf.at[:, pl.ds(mine, 64)], part_sem.at[0], part_sem.at[1],
        device_id=(1 - c, g), device_id_type=MESH,
    )
    part.start()
    for to in line(2):
        signal(meet.at[0], to)
    lane = lanes((CHUNK, 128))
    ROWS = range(0, 128, CHUNK)
    near = pl.multiple_of(128 - my_cols, 128)
    part.wait()
    for q in range(5):
        for rows in ROWS:
            here = pl.ds(rows, CHUNK)
            plain[q, here] = pltpu.roll(buf[q, here, pl.ds(my_cols, 128)], 32, 1)
            edge[q, here] = pltpu.roll(buf[q, here, pl.ds(near, 128)], 32, 1)

    def put(ref, at, rows, value):
        ref[at + (pl.ds(8 + rows, CHUNK),)] = value
        if rows == 0:
            ref[at + (pl.ds(136, 8),)] = value[:8]
        if rows == 128 - CHUNK:
            ref[at + (pl.ds(0, 8),)] = value[CHUNK - 8 :]

    def operate(slot, tile, rows):
        here = pl.ds(rows, CHUNK)
        centre = field[slot, tile, pl.ds(8 + rows, CHUNK)]
        total = coef[0, here] * centre
        for number, (offset, _, _) in enumerate(STENCIL):
            total = total + coef[1 + number, here] * field[slot, tile, pl.ds(8 + rows + offset, CHUNK)]
        for number, (offset, _, _) in enumerate(STENCIL):
            total = total + coef[5 + number, here] * pltpu.roll(centre, (-offset) % 128, 1)
        return centre, total

    def half(phase, carry):
        tile = lax.rem(1 - c + phase, 2)

        @pl.when(phase == 1)
        def _():
            for side in range(2):
                pltpu.make_async_copy(halo.at[side], halo.at[side], halo_sem.at[side]).wait()
            for side in range(2):
                for q in range(4):
                    far = halo[side, pl.ds(0, 64)]
                    edge[q, pl.ds(64 * side, 64)] = pltpu.roll(far, 128 - 32 * q, 1) if q else far
                for q in range(4):
                    far = halo[side, pl.ds(64, 16)]
                    edge[4, pl.ds(64 * side + 16 * q, 16)] = pltpu.roll(far, 128 - 32 * q, 1) if q else far
            pl.semaphore_wait(meet.at[0], sizes[2] - 1)
            for to in line(1):
                signal(meet.at[1], to)

        halo_lanes = (lane >= 32 * tile) & (lane < 32 * tile + 32)
        core_lanes = ((lane >= 32) & (lane < 96)).astype(jnp.int32) == 1 - tile

        def gather(q, rows):
            here = pl.ds(rows, CHUNK)
            return jnp.where(halo_lanes, edge[q, here], plain[q, here])

        for rows in ROWS:
            put(field, (0, tile), rows, gather(1, rows))
            put(speed, (), rows, gather(3, rows))
        for rows in ROWS:
            here = pl.ds(rows, CHUNK)
            coef[0, here] = SCALE * (gather(2, rows) + 5.0)
            vx = speed[pl.ds(8 + rows, CHUNK)]
            for number, (offset, flat, slope) in enumerate(STENCIL):
                other = speed[pl.ds(8 + rows + offset, CHUNK)]
                coef[1 + number, here] = flat + slope * (vx + other)
            vy = gather(4, rows)
            for number, (offset, flat, slope) in enumerate(STENCIL):
                other = pltpu.roll(vy, (-offset) % 128, 1)
                coef[5 + number, here] = flat + slope * (vy + other)
        for rows in ROWS:
            _, total = operate(0, tile, rows)
            value = gather(0, rows) - (1.0 / SCALE) * total
            put(field, (1, tile), rows, value)
            pltpu.store(image.at[STEPS, pl.ds(rows, CHUNK)], value, mask=core_lanes)

        def step(k, carry):
            centre_k = table[0, k]
            link_k = table[1, k]
            for rows in ROWS:
                now, total = operate(k + 1, tile, rows)
                before = field[k, tile, pl.ds(8 + rows, CHUNK)]
                put(field, (k + 2, tile), rows, total - centre_k * now - link_k * before)
                pltpu.store(image.at[k, pl.ds(rows, CHUNK)], total, mask=core_lanes)
            return carry

        return lax.fori_loop(0, STEPS, step, carry)

    lax.fori_loop(0, 2, half, 0)

    def core(lane, first, second):
        return jnp.where((lane >= 32) & (lane < 96), first, second)

    for number, (bi, bj) in enumerate(BLOCKS):

        def products(row, sums, bi=bi, bj=bj):
            for part in range(4):
                at = pl.ds(pl.multiple_of(row * 32 + 8 * part, 8), 8)
                left = [image[4 * bi + a, at] for a in range(4)]
                right = left if bi == bj else [image[4 * bj + b, at] for b in range(4)]
                sums = tuple(sums[4 * a + b] + left[a] * right[b] for a in range(4) for b in range(4))
            return sums

        sums = lax.fori_loop(0, 4, products, (jnp.zeros((8, 128), F32),) * 16)
        for a in range(16):
            acc[number * 16 + a] = sums[a]

    totals = jnp.sum(jnp.sum(acc[...], axis=1), axis=1, keepdims=True)
    wide = jnp.broadcast_to(totals[:128], (128, 128))
    pick = lax.broadcasted_iota(jnp.int32, (128, 128), 0) == lanes((128, 128))
    msg[pl.ds(0, 1)] = jnp.sum(jnp.where(pick, wide, 0.0), axis=0, keepdims=True)
    wide = jnp.broadcast_to(totals[128:], (32, 128))
    msg[pl.ds(1, 1)] = jnp.sum(jnp.where(pick[:32], wide, 0.0), axis=0, keepdims=True)

    pl.semaphore_wait(meet.at[1], sizes[1] - 1)

    def hops(way):
        return sum(min(k, size - k) for k, size in zip(way[:3], sizes)) + 0.5 * way[3]

    ways = [(z, y, x, w) for z in range(sizes[0]) for y in range(sizes[1]) for x in range(sizes[2]) for w in range(2)]
    for z, y, x, w in sorted(ways[1:], key=hops, reverse=True):
        pltpu.make_async_remote_copy(
            msg, every.at[me], sum_sem.at[0], sum_sem.at[1],
            device_id=(1 - c if w else c, around[0][z] + around[1][y] + around[2][x]), device_id_type=MESH,
        ).start()
    every[me] = msg[...]
    others = every.at[pl.ds(0, n - 1)]
    pltpu.make_async_copy(others, others, sum_sem.at[1]).wait()
    width = n // 2
    total = every[pl.ds(0, width)] + every[pl.ds(width, width)]
    while width > 1:
        width //= 2
        total = total[:width] + total[width:]
    total = total[0]

    wide = jnp.where(pick, jnp.broadcast_to(total[0:1], (128, 128)), 0.0)
    spread[pl.ds(0, 128)] = jnp.broadcast_to(jnp.sum(wide, axis=1, keepdims=True), (128, 128))
    wide = jnp.where(pick[:32], jnp.broadcast_to(total[1:2], (32, 128)), 0.0)
    spread[pl.ds(128, 32)] = jnp.broadcast_to(jnp.sum(wide, axis=1, keepdims=True), (32, 128))

    def entry(i, j):
        at = SLOT[(min(i, j), max(i, j))]
        return jnp.broadcast_to(spread[at : at + 1], (8, 128))

    gram = [[entry(i, j) for j in range(i + 1)] for i in range(STEPS)]
    goal = [entry(i, STEPS) for i in range(STEPS)]
    inverse = []
    for k in range(STEPS):
        inverse.append(1.0 / gram[k][k])
        for i in range(k + 1, STEPS):
            ratio = gram[i][k] * inverse[k]
            for j in range(k + 1, i + 1):
                gram[i][j] = gram[i][j] - ratio * gram[j][k]
            goal[i] = goal[i] - ratio * goal[k]
    weights = [None] * STEPS
    for k in reversed(range(STEPS)):
        value = goal[k]
        for i in range(k + 1, STEPS):
            value = value - gram[i][k] * weights[i]
        weights[k] = value * inverse[k]

    lane8 = lanes((8, 128))
    inside = (lane8 >= 32) & (lane8 < 96)

    def finish(first):
        def some(row, carry):
            for part in range(4):
                at = pl.ds(pl.multiple_of(first + row * 32 + 8 * part, 8), 8)
                inner = pl.ds(pl.multiple_of(first + row * 32 + 8 * part + 8, 8), 8)
                leftover = image[STEPS, at]
                change = None
                for k in range(STEPS):
                    leftover = leftover - weights[k] * image[k, at]
                    term = weights[k] * jnp.where(inside, field[k + 1, 0, inner], field[k + 1, 1, inner])
                    change = term if change is None else change + term
                start = jnp.where(inside, field[0, 0, inner], field[0, 1, inner])
                done[0, at] = pltpu.roll(start + SCALE * change, 96, 1)
                done[1, at] = pltpu.roll(leftover, 96, 1)
            return carry

        lax.fori_loop(0, 2, some, 0)

    finish(theirs)
    aways = []
    for o in range(2):
        away = pltpu.make_async_remote_copy(
            done.at[o, pl.ds(theirs, 64)], outs[o].at[:, pl.ds(my_cols, 128)], far_sem.at[0, o], far_sem.at[1, o],
            device_id=(1 - c, g), device_id_type=MESH,
        )
        away.start()
        aways.append(away)
    finish(mine)
    for o in range(2):
        outs[o][:, pl.ds(my_cols, 128)] = done[o, pl.ds(mine, 64)]
    for away in aways:
        away.wait()
    for edge_copy in edges:
        edge_copy.wait_send()
    pltpu.make_async_copy(others, others, sum_sem.at[0]).wait()


STENCIL = [
    (-2, SCALE / 12.0, SCALE / 24.0),
    (-1, -SCALE * 16.0 / 12.0, -SCALE * 8.0 / 24.0),
    (1, -SCALE * 16.0 / 12.0, SCALE * 8.0 / 24.0),
    (2, SCALE / 12.0, -SCALE / 24.0),
]


def write(*refs):
    moves = [pltpu.make_async_copy(refs[o], refs[2 + o], refs[4].at[o]) for o in range(2)]
    for move in moves:
        move.start()
    for move in moves:
        move.wait()


def solution(mesh):
    gy = mesh.shape["gy"]
    n = 2 * gy
    anywhere = pl.BlockSpec(memory_space=pl.ANY)

    def per_device(*blocks):
        blocks = [pltpu.with_memory_space_constraint(block, pltpu.HBM) for block in blocks]
        both = pl.pallas_call(
            functools.partial(kernel, gy),
            out_shape=[jax.ShapeDtypeStruct((64, 256), F32)] * 2,
            in_specs=[anywhere] * 5,
            out_specs=[pl.BlockSpec(memory_space=pltpu.VMEM)] * 2,
            scratch_shapes=[
                pltpu.VMEM((5, 128, 256), F32),
                pltpu.VMEM((2, 80, 128), F32),
                pltpu.VMEM((2, 80, 128), F32),
                pltpu.VMEM((5, 128, 128), F32),
                pltpu.VMEM((5, 128, 128), F32),
                pltpu.VMEM((144, 128), F32),
                pltpu.VMEM((9, 128, 128), F32),
                pltpu.VMEM((STEPS + 2, 2, 144, 128), F32),
                pltpu.VMEM((STEPS + 1, 128, 128), F32),
                pltpu.VMEM((160, 8, 128), F32),
                pltpu.VMEM((2, 128), F32),
                pltpu.VMEM((n, 2, 128), F32),
                pltpu.VMEM((160, 128), F32),
                pltpu.VMEM((2, 128, 128), F32),
                pltpu.SMEM((2, 16), F32),
                pltpu.SemaphoreType.DMA((5,)),
                pltpu.SemaphoreType.DMA((2,)),
                pltpu.SemaphoreType.DMA((2,)),
                pltpu.SemaphoreType.DMA((2,)),
                pltpu.SemaphoreType.DMA((2,)),
                pltpu.SemaphoreType.DMA((2, 2)),
                pltpu.SemaphoreType.REGULAR((2,)),
            ],
            compiler_params=pltpu.CompilerParams(collective_id=0, has_side_effects=True, vmem_limit_bytes=12 << 20),
        )(*blocks)
        return pl.pallas_call(
            write,
            out_shape=[jax.ShapeDtypeStruct((64, 256), F32)] * 2,
            in_specs=[anywhere] * 2,
            out_specs=[anywhere] * 2,
            scratch_shapes=[pltpu.SemaphoreType.DMA((2,))],
        )(*[pltpu.with_memory_space_constraint(one, pltpu.VMEM) for one in both])

    placed = P("gx", "gy")
    return jax.shard_map(
        per_device, mesh=mesh, in_specs=(placed,) * 5, out_specs=(placed, placed), check_vma=False
    )
```

```python
import functools

import jax
import jax.numpy as jnp
import numpy as np
from jax import lax
from jax.experimental import pallas as pl
from jax.experimental.pallas import tpu as pltpu
from jax.sharding import PartitionSpec as P

MESH = pl.DeviceIdType.MESH
STEPS = 15
CHUNK = 32
F32 = jnp.float32


def recurrence():
    count = 128
    angle = (np.arange(count) + 0.5) * np.pi / count
    one = (30.0 - 32.0 * np.cos(angle) + 2.0 * np.cos(2.0 * angle)) / 12.0
    values = (0.2 + one[:, None] + one[None, :]).ravel()
    weight = values * values
    scale = 4.0 / (values.max() - values.min())
    values = values * scale
    before, now, norm_before = np.zeros_like(values), np.ones_like(values), 1.0
    centres, links = [], []
    for k in range(STEPS):
        norm = (weight * now * now).sum()
        centre = (weight * values * now * now).sum() / norm
        link = norm / norm_before if k else 0.0
        centres.append(float(centre))
        links.append(float(link))
        before, now, norm_before = now, (values - centre) * now - link * before, norm
    return float(scale), centres, links


SCALE, CENTRES, LINKS = recurrence()

BLOCKS = [(i, j) for i in range(4) for j in range(i, 4)]
SLOT = {}
for number, (bi, bj) in enumerate(BLOCKS):
    for a in range(4):
        for b in range(4):
            SLOT.setdefault((4 * bi + a, 4 * bj + b), number * 16 + a * 4 + b)


def lanes(shape):
    return lax.broadcasted_iota(jnp.int32, shape, 1)


def kernel(gy, *refs):
    ins, outs = refs[:5], refs[5:7]
    (buf, send, halo, plain, edge, speed, coef, field, image, acc, msg, every, spread, done, table,
     in_sem, part_sem, edge_sem, halo_sem, sum_sem, far_sem, meet) = refs[7:]
    c = lax.axis_index("gx")
    g = lax.axis_index("gy")
    n = 2 * gy
    me = c * gy + g
    mine = pl.multiple_of(c * 64, 64)
    theirs = pl.multiple_of((1 - c) * 64, 64)
    my_cols = pl.multiple_of(c * 128, 128)

    loads = [pltpu.make_async_copy(ins[q], buf.at[q, pl.ds(mine, 64)], in_sem.at[q]) for q in range(5)]
    for load in loads:
        load.start()

    sizes = (4, 4, 4) if gy == 64 else (1, 2, gy // 2)
    strides = (sizes[1] * sizes[2], sizes[2], 1)
    around = [
        [lax.rem(lax.rem(g // stride, size) + k, size) * stride for k in range(size)]
        for stride, size in zip(strides, sizes)
    ]
    ahead, behind = lax.rem(g + 1, gy), lax.rem(g + gy - 1, gy)

    def line(d):
        rest = g - around[d][0]
        return [(c, rest + around[d][k]) for k in sorted(range(1, sizes[d]), key=lambda k: k != sizes[d] // 2)]

    def signal(sem, to):
        pl.semaphore_signal(sem, inc=1, device_id=to, device_id_type=MESH)

    barrier = pltpu.get_barrier_semaphore()
    sender = jnp.where(c == 0, behind, ahead)
    across = [(1 - c, chip) for _, chip in line(0)]
    greeted = [(0, sender), (1, sender)] + line(0) + across + line(1) + line(2) + [(1 - c, g)]
    for to in greeted:
        signal(barrier, to)

    for k in range(STEPS):
        table[0, k] = CENTRES[k]
        table[1, k] = LINKS[k]
    for load in loads:
        load.wait()

    lane64 = lanes((64, 128))
    lane16 = lanes((16, 128))
    for way in range(2):
        tile, first = (1, 96) if way == 0 else (0, 0)
        packed = None
        for q in range(4):
            at = 32 * (q if way == 0 else (q + 1) % 4)
            piece = buf[q, pl.ds(mine, 64), pl.ds(128 * tile, 128)]
            shift = (at - first) % 128
            piece = pltpu.roll(piece, shift, 1) if shift else piece
            packed = piece if packed is None else jnp.where((lane64 >= at) & (lane64 < at + 32), piece, packed)
        send[way, pl.ds(0, 64)] = packed
        packed = None
        for q in range(4):
            at = 32 * (q if way == 0 else (q + 1) % 4)
            piece = buf[4, pl.ds(pl.multiple_of(mine + 16 * q, 16), 16), pl.ds(128 * tile, 128)]
            shift = (at - first) % 128
            piece = pltpu.roll(piece, shift, 1) if shift else piece
            packed = piece if packed is None else jnp.where((lane16 >= at) & (lane16 < at + 32), piece, packed)
        send[way, pl.ds(64, 16)] = packed

    pl.semaphore_wait(barrier, len(greeted))

    edges = []
    for way, (core, chip) in enumerate(((0, ahead), (1, behind))):
        copy = pltpu.make_async_remote_copy(
            send.at[way], halo.at[c], edge_sem.at[way], halo_sem.at[c], device_id=(core, chip), device_id_type=MESH
        )
        copy.start()
        edges.append(copy)
    part = pltpu.make_async_remote_copy(
        buf.at[:, pl.ds(mine, 64)], buf.at[:, pl.ds(mine, 64)], part_sem.at[0], part_sem.at[1],
        device_id=(1 - c, g), device_id_type=MESH,
    )
    part.start()
    for to in line(2):
        signal(meet.at[0], to)
    lane = lanes((CHUNK, 128))
    ROWS = range(0, 128, CHUNK)
    near = pl.multiple_of(128 - my_cols, 128)
    part.wait()
    for q in range(5):
        for rows in ROWS:
            here = pl.ds(rows, CHUNK)
            plain[q, here] = pltpu.roll(buf[q, here, pl.ds(my_cols, 128)], 32, 1)
            edge[q, here] = pltpu.roll(buf[q, here, pl.ds(near, 128)], 32, 1)

    def put(ref, at, rows, value):
        ref[at + (pl.ds(8 + rows, CHUNK),)] = value
        if rows == 0:
            ref[at + (pl.ds(136, 8),)] = value[:8]
        if rows == 128 - CHUNK:
            ref[at + (pl.ds(0, 8),)] = value[CHUNK - 8 :]

    def operate(slot, tile, rows, centre):
        here = pl.ds(rows, CHUNK)
        turned = [
            coef[5 + number, here] * pltpu.roll(centre, (-offset) % 128, 1)
            for number, (offset, _, _) in enumerate(STENCIL)
        ]
        moved = [
            coef[1 + number, here] * field[slot, tile, pl.ds(8 + rows + offset, CHUNK)]
            for number, (offset, _, _) in enumerate(STENCIL)
        ]
        still = coef[0, here] * centre + ((moved[0] + moved[1]) + (moved[2] + moved[3]))
        return still, (turned[0] + turned[1]) + (turned[2] + turned[3])

    def half(phase, carry):
        tile = lax.rem(1 - c + phase, 2)

        @pl.when(phase == 1)
        def _():
            for side in range(2):
                pltpu.make_async_copy(halo.at[side], halo.at[side], halo_sem.at[side]).wait()
            for side in range(2):
                for q in range(4):
                    far = halo[side, pl.ds(0, 64)]
                    edge[q, pl.ds(64 * side, 64)] = pltpu.roll(far, 128 - 32 * q, 1) if q else far
                for q in range(4):
                    far = halo[side, pl.ds(64, 16)]
                    edge[4, pl.ds(64 * side + 16 * q, 16)] = pltpu.roll(far, 128 - 32 * q, 1) if q else far
            pl.semaphore_wait(meet.at[0], sizes[2] - 1)
            for to in line(1):
                signal(meet.at[1], to)

        halo_lanes = (lane >= 32 * tile) & (lane < 32 * tile + 32)
        core_lanes = ((lane >= 32) & (lane < 96)).astype(jnp.int32) == 1 - tile

        def gather(q, rows):
            here = pl.ds(rows, CHUNK)
            return jnp.where(halo_lanes, edge[q, here], plain[q, here])

        for rows in ROWS:
            put(field, (0, tile), rows, gather(1, rows))
            put(speed, (), rows, gather(3, rows))
        for rows in ROWS:
            here = pl.ds(rows, CHUNK)
            coef[0, here] = SCALE * (gather(2, rows) + 5.0)
            vx = speed[pl.ds(8 + rows, CHUNK)]
            for number, (offset, flat, slope) in enumerate(STENCIL):
                other = speed[pl.ds(8 + rows + offset, CHUNK)]
                coef[1 + number, here] = flat + slope * (vx + other)
            vy = gather(4, rows)
            for number, (offset, flat, slope) in enumerate(STENCIL):
                other = pltpu.roll(vy, (-offset) % 128, 1)
                coef[5 + number, here] = flat + slope * (vy + other)
        for rows in ROWS:
            still, turned = operate(0, tile, rows, field[0, tile, pl.ds(8 + rows, CHUNK)])
            value = gather(0, rows) - (1.0 / SCALE) * (still + turned)
            put(field, (1, tile), rows, value)
            pltpu.store(image.at[STEPS, pl.ds(rows, CHUNK)], value, mask=core_lanes)

        def steps(turn, carry):
            centres = None
            for k in [turn * 5 + part for part in range(5)]:
                centre_k = table[0, k]
                link_k = table[1, k]
                afters = []
                for index, rows in enumerate(ROWS):
                    now = centres[index] if centres else field[k + 1, tile, pl.ds(8 + rows, CHUNK)]
                    still, turned = operate(k + 1, tile, rows, now)
                    before = field[k, tile, pl.ds(8 + rows, CHUNK)]
                    rest = still - centre_k * now - link_k * before
                    after = rest + turned
                    put(field, (k + 2, tile), rows, after)
                    pltpu.store(image.at[k, pl.ds(rows, CHUNK)], still + turned, mask=core_lanes)
                    afters.append(after)
                centres = afters
            return carry

        return lax.fori_loop(0, STEPS // 5, steps, carry)

    lax.fori_loop(0, 2, half, 0)

    def core(lane, first, second):
        return jnp.where((lane >= 32) & (lane < 96), first, second)

    for number, (bi, bj) in enumerate(BLOCKS):

        def products(row, sums, bi=bi, bj=bj):
            for part in range(4):
                at = pl.ds(pl.multiple_of(row * 32 + 8 * part, 8), 8)
                left = [image[4 * bi + a, at] for a in range(4)]
                right = left if bi == bj else [image[4 * bj + b, at] for b in range(4)]
                sums = tuple(sums[4 * a + b] + left[a] * right[b] for a in range(4) for b in range(4))
            return sums

        sums = lax.fori_loop(0, 4, products, (jnp.zeros((8, 128), F32),) * 16)
        for a in range(16):
            acc[number * 16 + a] = sums[a]

    totals = jnp.sum(jnp.sum(acc[...], axis=1), axis=1, keepdims=True)
    wide = jnp.broadcast_to(totals[:128], (128, 128))
    pick = lax.broadcasted_iota(jnp.int32, (128, 128), 0) == lanes((128, 128))
    msg[pl.ds(0, 1)] = jnp.sum(jnp.where(pick, wide, 0.0), axis=0, keepdims=True)
    wide = jnp.broadcast_to(totals[128:], (32, 128))
    msg[pl.ds(1, 1)] = jnp.sum(jnp.where(pick[:32], wide, 0.0), axis=0, keepdims=True)

    pl.semaphore_wait(meet.at[1], sizes[1] - 1)

    def hops(way):
        return sum(min(k, size - k) for k, size in zip(way[:3], sizes)) + 0.5 * way[3]

    ways = [(z, y, x, w) for z in range(sizes[0]) for y in range(sizes[1]) for x in range(sizes[2]) for w in range(2)]
    for z, y, x, w in sorted(ways[1:], key=hops, reverse=True):
        pltpu.make_async_remote_copy(
            msg, every.at[me], sum_sem.at[0], sum_sem.at[1],
            device_id=(1 - c if w else c, around[0][z] + around[1][y] + around[2][x]), device_id_type=MESH,
        ).start()
    every[me] = msg[...]
    others = every.at[pl.ds(0, n - 1)]
    pltpu.make_async_copy(others, others, sum_sem.at[1]).wait()
    width = n // 2
    total = every[pl.ds(0, width)] + every[pl.ds(width, width)]
    while width > 1:
        width //= 2
        total = total[:width] + total[width:]
    total = total[0]

    wide = jnp.where(pick, jnp.broadcast_to(total[0:1], (128, 128)), 0.0)
    spread[pl.ds(0, 128)] = jnp.broadcast_to(jnp.sum(wide, axis=1, keepdims=True), (128, 128))
    wide = jnp.where(pick[:32], jnp.broadcast_to(total[1:2], (32, 128)), 0.0)
    spread[pl.ds(128, 32)] = jnp.broadcast_to(jnp.sum(wide, axis=1, keepdims=True), (32, 128))

    def entry(i, j):
        at = SLOT[(min(i, j), max(i, j))]
        return jnp.broadcast_to(spread[at : at + 1], (8, 128))

    gram = [[entry(i, j) for j in range(i + 1)] for i in range(STEPS)]
    goal = [entry(i, STEPS) for i in range(STEPS)]
    inverse = []
    for k in range(STEPS):
        inverse.append(1.0 / gram[k][k])
        for i in range(k + 1, STEPS):
            ratio = gram[i][k] * inverse[k]
            for j in range(k + 1, i + 1):
                gram[i][j] = gram[i][j] - ratio * gram[j][k]
            goal[i] = goal[i] - ratio * goal[k]
    weights = [None] * STEPS
    for k in reversed(range(STEPS)):
        value = goal[k]
        for i in range(k + 1, STEPS):
            value = value - gram[i][k] * weights[i]
        weights[k] = value * inverse[k]

    lane8 = lanes((8, 128))
    inside = (lane8 >= 32) & (lane8 < 96)

    def finish(first):
        def some(row, carry):
            for part in range(4):
                at = pl.ds(pl.multiple_of(first + row * 32 + 8 * part, 8), 8)
                inner = pl.ds(pl.multiple_of(first + row * 32 + 8 * part + 8, 8), 8)
                leftover = image[STEPS, at]
                change = None
                for k in range(STEPS):
                    leftover = leftover - weights[k] * image[k, at]
                    term = weights[k] * jnp.where(inside, field[k + 1, 0, inner], field[k + 1, 1, inner])
                    change = term if change is None else change + term
                start = jnp.where(inside, field[0, 0, inner], field[0, 1, inner])
                done[0, at] = pltpu.roll(start + SCALE * change, 96, 1)
                done[1, at] = pltpu.roll(leftover, 96, 1)
            return carry

        lax.fori_loop(0, 2, some, 0)

    finish(theirs)
    aways = []
    for o in range(2):
        away = pltpu.make_async_remote_copy(
            done.at[o, pl.ds(theirs, 64)], outs[o].at[:, pl.ds(my_cols, 128)], far_sem.at[0, o], far_sem.at[1, o],
            device_id=(1 - c, g), device_id_type=MESH,
        )
        away.start()
        aways.append(away)
    finish(mine)
    for o in range(2):
        outs[o][:, pl.ds(my_cols, 128)] = done[o, pl.ds(mine, 64)]
    for away in aways:
        away.wait()
    for edge_copy in edges:
        edge_copy.wait_send()
    pltpu.make_async_copy(others, others, sum_sem.at[0]).wait()


STENCIL = [
    (-2, SCALE / 12.0, SCALE / 24.0),
    (-1, -SCALE * 16.0 / 12.0, -SCALE * 8.0 / 24.0),
    (1, -SCALE * 16.0 / 12.0, SCALE * 8.0 / 24.0),
    (2, SCALE / 12.0, -SCALE / 24.0),
]


def write(*refs):
    moves = [pltpu.make_async_copy(refs[o], refs[2 + o], refs[4].at[o]) for o in range(2)]
    for move in moves:
        move.start()
    for move in moves:
        move.wait()


def solution(mesh):
    gy = mesh.shape["gy"]
    n = 2 * gy
    anywhere = pl.BlockSpec(memory_space=pl.ANY)

    def per_device(*blocks):
        blocks = [pltpu.with_memory_space_constraint(block, pltpu.HBM) for block in blocks]
        both = pl.pallas_call(
            functools.partial(kernel, gy),
            out_shape=[jax.ShapeDtypeStruct((64, 256), F32)] * 2,
            in_specs=[anywhere] * 5,
            out_specs=[pl.BlockSpec(memory_space=pltpu.VMEM)] * 2,
            scratch_shapes=[
                pltpu.VMEM((5, 128, 256), F32),
                pltpu.VMEM((2, 80, 128), F32),
                pltpu.VMEM((2, 80, 128), F32),
                pltpu.VMEM((5, 128, 128), F32),
                pltpu.VMEM((5, 128, 128), F32),
                pltpu.VMEM((144, 128), F32),
                pltpu.VMEM((9, 128, 128), F32),
                pltpu.VMEM((STEPS + 2, 2, 144, 128), F32),
                pltpu.VMEM((STEPS + 1, 128, 128), F32),
                pltpu.VMEM((160, 8, 128), F32),
                pltpu.VMEM((2, 128), F32),
                pltpu.VMEM((n, 2, 128), F32),
                pltpu.VMEM((160, 128), F32),
                pltpu.VMEM((2, 128, 128), F32),
                pltpu.SMEM((2, 16), F32),
                pltpu.SemaphoreType.DMA((5,)),
                pltpu.SemaphoreType.DMA((2,)),
                pltpu.SemaphoreType.DMA((2,)),
                pltpu.SemaphoreType.DMA((2,)),
                pltpu.SemaphoreType.DMA((2,)),
                pltpu.SemaphoreType.DMA((2, 2)),
                pltpu.SemaphoreType.REGULAR((2,)),
            ],
            compiler_params=pltpu.CompilerParams(collective_id=0, has_side_effects=True, vmem_limit_bytes=12 << 20),
        )(*blocks)
        return pl.pallas_call(
            write,
            out_shape=[jax.ShapeDtypeStruct((64, 256), F32)] * 2,
            in_specs=[anywhere] * 2,
            out_specs=[anywhere] * 2,
            scratch_shapes=[pltpu.SemaphoreType.DMA((2,))],
        )(*[pltpu.with_memory_space_constraint(one, pltpu.VMEM) for one in both])

    placed = P("gx", "gy")
    return jax.shard_map(
        per_device, mesh=mesh, in_specs=(placed,) * 5, out_specs=(placed, placed), check_vma=False
    )
```

```python
import functools

import jax
import jax.numpy as jnp
import numpy as np
from jax import lax
from jax.experimental import pallas as pl
from jax.experimental.pallas import tpu as pltpu
from jax.sharding import PartitionSpec as P

MESH = pl.DeviceIdType.MESH
STEPS = 15
CHUNK = 32
F32 = jnp.float32


def recurrence():
    count = 128
    angle = (np.arange(count) + 0.5) * np.pi / count
    one = (30.0 - 32.0 * np.cos(angle) + 2.0 * np.cos(2.0 * angle)) / 12.0
    values = (0.2 + one[:, None] + one[None, :]).ravel()
    weight = values * values
    scale = 4.0 / (values.max() - values.min())
    values = values * scale
    before, now, norm_before = np.zeros_like(values), np.ones_like(values), 1.0
    centres, links = [], []
    for k in range(STEPS):
        norm = (weight * now * now).sum()
        centre = (weight * values * now * now).sum() / norm
        link = norm / norm_before if k else 0.0
        centres.append(float(centre))
        links.append(float(link))
        before, now, norm_before = now, (values - centre) * now - link * before, norm
    return float(scale), centres, links


SCALE, CENTRES, LINKS = recurrence()

BLOCKS = [(i, j) for i in range(4) for j in range(i, 4)]
SLOT = {}
for number, (bi, bj) in enumerate(BLOCKS):
    for a in range(4):
        for b in range(4):
            SLOT.setdefault((4 * bi + a, 4 * bj + b), number * 16 + a * 4 + b)


def lanes(shape):
    return lax.broadcasted_iota(jnp.int32, shape, 1)


def kernel(gy, *refs):
    ins, outs = refs[:5], refs[5:7]
    (buf, send, halo, plain, edge, speed, coef, field, image, acc, msg, every, spread, done, table,
     in_sem, part_sem, edge_sem, halo_sem, sum_sem, far_sem, meet) = refs[7:]
    c = lax.axis_index("gx")
    g = lax.axis_index("gy")
    n = 2 * gy
    me = c * gy + g
    mine = pl.multiple_of(c * 64, 64)
    theirs = pl.multiple_of((1 - c) * 64, 64)
    my_cols = pl.multiple_of(c * 128, 128)

    loads = [pltpu.make_async_copy(ins[q], buf.at[q, pl.ds(mine, 64)], in_sem.at[q]) for q in range(5)]
    for load in loads:
        load.start()

    sizes = (4, 4, 4) if gy == 64 else (1, 2, gy // 2)
    strides = (sizes[1] * sizes[2], sizes[2], 1)
    around = [
        [lax.rem(lax.rem(g // stride, size) + k, size) * stride for k in range(size)]
        for stride, size in zip(strides, sizes)
    ]
    ahead, behind = lax.rem(g + 1, gy), lax.rem(g + gy - 1, gy)

    def line(d):
        rest = g - around[d][0]
        return [(c, rest + around[d][k]) for k in sorted(range(1, sizes[d]), key=lambda k: k != sizes[d] // 2)]

    def signal(sem, to):
        pl.semaphore_signal(sem, inc=1, device_id=to, device_id_type=MESH)

    barrier = pltpu.get_barrier_semaphore()
    sender = jnp.where(c == 0, behind, ahead)
    across = [(1 - c, chip) for _, chip in line(0)]
    greeted = [(0, sender), (1, sender)] + line(0) + across + line(1) + line(2) + [(1 - c, g)]
    for to in greeted:
        signal(barrier, to)

    for k in range(STEPS):
        table[0, k] = CENTRES[k]
        table[1, k] = LINKS[k]
    for load in loads:
        load.wait()

    lane64 = lanes((64, 128))
    lane16 = lanes((16, 128))
    for way in range(2):
        tile, first = (1, 96) if way == 0 else (0, 0)
        packed = None
        for q in range(4):
            at = 32 * (q if way == 0 else (q + 1) % 4)
            piece = buf[q, pl.ds(mine, 64), pl.ds(128 * tile, 128)]
            shift = (at - first) % 128
            piece = pltpu.roll(piece, shift, 1) if shift else piece
            packed = piece if packed is None else jnp.where((lane64 >= at) & (lane64 < at + 32), piece, packed)
        send[way, pl.ds(0, 64)] = packed
        packed = None
        for q in range(4):
            at = 32 * (q if way == 0 else (q + 1) % 4)
            piece = buf[4, pl.ds(pl.multiple_of(mine + 16 * q, 16), 16), pl.ds(128 * tile, 128)]
            shift = (at - first) % 128
            piece = pltpu.roll(piece, shift, 1) if shift else piece
            packed = piece if packed is None else jnp.where((lane16 >= at) & (lane16 < at + 32), piece, packed)
        send[way, pl.ds(64, 16)] = packed

    pl.semaphore_wait(barrier, len(greeted))

    edges = []
    for way, (core, chip) in enumerate(((0, ahead), (1, behind))):
        copy = pltpu.make_async_remote_copy(
            send.at[way], halo.at[c], edge_sem.at[way], halo_sem.at[c], device_id=(core, chip), device_id_type=MESH
        )
        copy.start()
        edges.append(copy)
    part = pltpu.make_async_remote_copy(
        buf.at[:, pl.ds(mine, 64)], buf.at[:, pl.ds(mine, 64)], part_sem.at[0], part_sem.at[1],
        device_id=(1 - c, g), device_id_type=MESH,
    )
    part.start()
    for to in line(2):
        signal(meet.at[0], to)
    lane = lanes((CHUNK, 128))
    ROWS = range(0, 128, CHUNK)
    near = pl.multiple_of(128 - my_cols, 128)

    def turn_in(first):
        for q in range(5):
            for rows in range(0, 64, CHUNK):
                here = pl.ds(pl.multiple_of(first + rows, CHUNK), CHUNK)
                plain[q, here] = pltpu.roll(buf[q, here, pl.ds(my_cols, 128)], 32, 1)
                edge[q, here] = pltpu.roll(buf[q, here, pl.ds(near, 128)], 32, 1)

    turn_in(mine)
    part.wait_recv()
    turn_in(theirs)

    def put(ref, at, rows, value):
        ref[at + (pl.ds(8 + rows, CHUNK),)] = value
        if rows == 0:
            ref[at + (pl.ds(136, 8),)] = value[:8]
        if rows == 128 - CHUNK:
            ref[at + (pl.ds(0, 8),)] = value[CHUNK - 8 :]

    def operate(slot, tile, rows, centre):
        here = pl.ds(rows, CHUNK)
        turned = [
            coef[5 + number, here] * pltpu.roll(centre, (-offset) % 128, 1)
            for number, (offset, _, _) in enumerate(STENCIL)
        ]
        moved = [
            coef[1 + number, here] * field[slot, tile, pl.ds(8 + rows + offset, CHUNK)]
            for number, (offset, _, _) in enumerate(STENCIL)
        ]
        still = coef[0, here] * centre + ((moved[0] + moved[1]) + (moved[2] + moved[3]))
        return still, (turned[0] + turned[1]) + (turned[2] + turned[3])

    def half(phase, carry):
        tile = lax.rem(1 - c + phase, 2)

        @pl.when(phase == 1)
        def _():
            for side in range(2):
                pltpu.make_async_copy(halo.at[side], halo.at[side], halo_sem.at[side]).wait()
            for side in range(2):
                for q in range(4):
                    far = halo[side, pl.ds(0, 64)]
                    edge[q, pl.ds(64 * side, 64)] = pltpu.roll(far, 128 - 32 * q, 1) if q else far
                for q in range(4):
                    far = halo[side, pl.ds(64, 16)]
                    edge[4, pl.ds(64 * side + 16 * q, 16)] = pltpu.roll(far, 128 - 32 * q, 1) if q else far

        halo_lanes = (lane >= 32 * tile) & (lane < 32 * tile + 32)
        core_lanes = ((lane >= 32) & (lane < 96)).astype(jnp.int32) == 1 - tile

        def gather(q, rows):
            here = pl.ds(rows, CHUNK)
            return jnp.where(halo_lanes, edge[q, here], plain[q, here])

        for rows in ROWS:
            put(field, (0, tile), rows, gather(1, rows))
            put(speed, (), rows, gather(3, rows))
        for rows in ROWS:
            here = pl.ds(rows, CHUNK)
            coef[0, here] = SCALE * (gather(2, rows) + 5.0)
            vx = speed[pl.ds(8 + rows, CHUNK)]
            for number, (offset, flat, slope) in enumerate(STENCIL):
                other = speed[pl.ds(8 + rows + offset, CHUNK)]
                coef[1 + number, here] = flat + slope * (vx + other)
            vy = gather(4, rows)
            for number, (offset, flat, slope) in enumerate(STENCIL):
                other = pltpu.roll(vy, (-offset) % 128, 1)
                coef[5 + number, here] = flat + slope * (vy + other)
        for rows in ROWS:
            still, turned = operate(0, tile, rows, field[0, tile, pl.ds(8 + rows, CHUNK)])
            value = gather(0, rows) - (1.0 / SCALE) * (still + turned)
            put(field, (1, tile), rows, value)
            pltpu.store(image.at[STEPS, pl.ds(rows, CHUNK)], value, mask=core_lanes)

        def steps(turn, carry):
            centres = None
            for k in [turn * 5 + part for part in range(5)]:
                centre_k = table[0, k]
                link_k = table[1, k]
                afters = []
                for index, rows in enumerate(ROWS):
                    now = centres[index] if centres else field[k + 1, tile, pl.ds(8 + rows, CHUNK)]
                    still, turned = operate(k + 1, tile, rows, now)
                    before = field[k, tile, pl.ds(8 + rows, CHUNK)]
                    rest = still - centre_k * now - link_k * before
                    after = rest + turned
                    put(field, (k + 2, tile), rows, after)
                    pltpu.store(image.at[k, pl.ds(rows, CHUNK)], still + turned, mask=core_lanes)
                    afters.append(after)
                centres = afters
            return carry

        return lax.fori_loop(0, STEPS // 5, steps, carry)

    lax.fori_loop(0, 1, half, 0)
    pl.semaphore_wait(meet.at[0], sizes[2] - 1)
    for to in line(1):
        signal(meet.at[1], to)
    lax.fori_loop(1, 2, half, 0)

    def core(lane, first, second):
        return jnp.where((lane >= 32) & (lane < 96), first, second)

    for number, (bi, bj) in enumerate(BLOCKS):

        def products(row, sums, bi=bi, bj=bj):
            for part in range(8):
                at = pl.ds(pl.multiple_of(row * 64 + 8 * part, 8), 8)
                left = [image[4 * bi + a, at] for a in range(4)]
                right = left if bi == bj else [image[4 * bj + b, at] for b in range(4)]
                sums = tuple(sums[4 * a + b] + left[a] * right[b] for a in range(4) for b in range(4))
            return sums

        sums = lax.fori_loop(0, 2, products, (jnp.zeros((8, 128), F32),) * 16)
        for a in range(16):
            acc[number * 16 + a] = sums[a]

    totals = jnp.sum(jnp.sum(acc[...], axis=1), axis=1, keepdims=True)
    wide = jnp.broadcast_to(totals[:128], (128, 128))
    pick = lax.broadcasted_iota(jnp.int32, (128, 128), 0) == lanes((128, 128))
    msg[pl.ds(0, 1)] = jnp.sum(jnp.where(pick, wide, 0.0), axis=0, keepdims=True)
    wide = jnp.broadcast_to(totals[128:], (32, 128))
    msg[pl.ds(1, 1)] = jnp.sum(jnp.where(pick[:32], wide, 0.0), axis=0, keepdims=True)

    pl.semaphore_wait(meet.at[1], sizes[1] - 1)

    def hops(way):
        return sum(min(k, size - k) for k, size in zip(way[:3], sizes)) + 0.5 * way[3]

    ways = [(z, y, x, w) for z in range(sizes[0]) for y in range(sizes[1]) for x in range(sizes[2]) for w in range(2)]
    for z, y, x, w in sorted(ways[1:], key=hops, reverse=True):
        pltpu.make_async_remote_copy(
            msg, every.at[me], sum_sem.at[0], sum_sem.at[1],
            device_id=(1 - c if w else c, around[0][z] + around[1][y] + around[2][x]), device_id_type=MESH,
        ).start()
    every[me] = msg[...]
    others = every.at[pl.ds(0, n - 1)]
    pltpu.make_async_copy(others, others, sum_sem.at[1]).wait()
    width = n // 2
    total = every[pl.ds(0, width)] + every[pl.ds(width, width)]
    while width > 1:
        width //= 2
        total = total[:width] + total[width:]
    total = total[0]

    wide = jnp.where(pick, jnp.broadcast_to(total[0:1], (128, 128)), 0.0)
    spread[pl.ds(0, 128)] = jnp.broadcast_to(jnp.sum(wide, axis=1, keepdims=True), (128, 128))
    wide = jnp.where(pick[:32], jnp.broadcast_to(total[1:2], (32, 128)), 0.0)
    spread[pl.ds(128, 32)] = jnp.broadcast_to(jnp.sum(wide, axis=1, keepdims=True), (32, 128))

    def entry(i, j):
        at = SLOT[(min(i, j), max(i, j))]
        return jnp.broadcast_to(spread[at : at + 1], (8, 128))

    gram = [[entry(i, j) for j in range(i + 1)] for i in range(STEPS)]
    goal = [entry(i, STEPS) for i in range(STEPS)]
    inverse = []
    for k in range(STEPS):
        inverse.append(1.0 / gram[k][k])
        for i in range(k + 1, STEPS):
            ratio = gram[i][k] * inverse[k]
            for j in range(k + 1, i + 1):
                gram[i][j] = gram[i][j] - ratio * gram[j][k]
            goal[i] = goal[i] - ratio * goal[k]
    weights = [None] * STEPS
    for k in reversed(range(STEPS)):
        value = goal[k]
        for i in range(k + 1, STEPS):
            value = value - gram[i][k] * weights[i]
        weights[k] = value * inverse[k]

    lane8 = lanes((8, 128))
    inside = (lane8 >= 32) & (lane8 < 96)

    def finish(first):
        def some(row, carry):
            for part in range(4):
                at = pl.ds(pl.multiple_of(first + row * 32 + 8 * part, 8), 8)
                inner = pl.ds(pl.multiple_of(first + row * 32 + 8 * part + 8, 8), 8)
                leftover = image[STEPS, at]
                change = None
                for k in range(STEPS):
                    leftover = leftover - weights[k] * image[k, at]
                    term = weights[k] * jnp.where(inside, field[k + 1, 0, inner], field[k + 1, 1, inner])
                    change = term if change is None else change + term
                start = jnp.where(inside, field[0, 0, inner], field[0, 1, inner])
                done[0, at] = pltpu.roll(start + SCALE * change, 96, 1)
                done[1, at] = pltpu.roll(leftover, 96, 1)
            return carry

        lax.fori_loop(0, 2, some, 0)

    finish(theirs)
    aways = []
    for o in range(2):
        away = pltpu.make_async_remote_copy(
            done.at[o, pl.ds(theirs, 64)], outs[o].at[:, pl.ds(my_cols, 128)], far_sem.at[0, o], far_sem.at[1, o],
            device_id=(1 - c, g), device_id_type=MESH,
        )
        away.start()
        aways.append(away)
    finish(mine)
    for o in range(2):
        outs[o][:, pl.ds(my_cols, 128)] = done[o, pl.ds(mine, 64)]
    for away in aways:
        away.wait()
    part.wait_send()
    for edge_copy in edges:
        edge_copy.wait_send()
    pltpu.make_async_copy(others, others, sum_sem.at[0]).wait()


STENCIL = [
    (-2, SCALE / 12.0, SCALE / 24.0),
    (-1, -SCALE * 16.0 / 12.0, -SCALE * 8.0 / 24.0),
    (1, -SCALE * 16.0 / 12.0, SCALE * 8.0 / 24.0),
    (2, SCALE / 12.0, -SCALE / 24.0),
]


def write(*refs):
    moves = [pltpu.make_async_copy(refs[o], refs[2 + o], refs[4].at[o]) for o in range(2)]
    for move in moves:
        move.start()
    for move in moves:
        move.wait()


def solution(mesh):
    gy = mesh.shape["gy"]
    n = 2 * gy
    anywhere = pl.BlockSpec(memory_space=pl.ANY)

    def per_device(*blocks):
        blocks = [pltpu.with_memory_space_constraint(block, pltpu.HBM) for block in blocks]
        both = pl.pallas_call(
            functools.partial(kernel, gy),
            out_shape=[jax.ShapeDtypeStruct((64, 256), F32)] * 2,
            in_specs=[anywhere] * 5,
            out_specs=[pl.BlockSpec(memory_space=pltpu.VMEM)] * 2,
            scratch_shapes=[
                pltpu.VMEM((5, 128, 256), F32),
                pltpu.VMEM((2, 80, 128), F32),
                pltpu.VMEM((2, 80, 128), F32),
                pltpu.VMEM((5, 128, 128), F32),
                pltpu.VMEM((5, 128, 128), F32),
                pltpu.VMEM((144, 128), F32),
                pltpu.VMEM((9, 128, 128), F32),
                pltpu.VMEM((STEPS + 2, 2, 144, 128), F32),
                pltpu.VMEM((STEPS + 1, 128, 128), F32),
                pltpu.VMEM((160, 8, 128), F32),
                pltpu.VMEM((2, 128), F32),
                pltpu.VMEM((n, 2, 128), F32),
                pltpu.VMEM((160, 128), F32),
                pltpu.VMEM((2, 128, 128), F32),
                pltpu.SMEM((2, 16), F32),
                pltpu.SemaphoreType.DMA((5,)),
                pltpu.SemaphoreType.DMA((2,)),
                pltpu.SemaphoreType.DMA((2,)),
                pltpu.SemaphoreType.DMA((2,)),
                pltpu.SemaphoreType.DMA((2,)),
                pltpu.SemaphoreType.DMA((2, 2)),
                pltpu.SemaphoreType.REGULAR((2,)),
            ],
            compiler_params=pltpu.CompilerParams(collective_id=0, has_side_effects=True, vmem_limit_bytes=12 << 20),
        )(*blocks)
        return pl.pallas_call(
            write,
            out_shape=[jax.ShapeDtypeStruct((64, 256), F32)] * 2,
            in_specs=[anywhere] * 2,
            out_specs=[anywhere] * 2,
            scratch_shapes=[pltpu.SemaphoreType.DMA((2,))],
        )(*[pltpu.with_memory_space_constraint(one, pltpu.VMEM) for one in both])

    placed = P("gx", "gy")
    return jax.shard_map(
        per_device, mesh=mesh, in_specs=(placed,) * 5, out_specs=(placed, placed), check_vma=False
    )
```

```python
import functools

import jax
import jax.numpy as jnp
import numpy as np
from jax import lax
from jax.experimental import pallas as pl
from jax.experimental.pallas import tpu as pltpu
from jax.sharding import PartitionSpec as P

MESH = pl.DeviceIdType.MESH
STEPS = 15
CHUNK = 32
F32 = jnp.float32


def recurrence():
    count = 128
    angle = (np.arange(count) + 0.5) * np.pi / count
    one = (30.0 - 32.0 * np.cos(angle) + 2.0 * np.cos(2.0 * angle)) / 12.0
    values = (0.2 + one[:, None] + one[None, :]).ravel()
    weight = values * values
    scale = 4.0 / (values.max() - values.min())
    values = values * scale
    before, now, norm_before = np.zeros_like(values), np.ones_like(values), 1.0
    centres, links = [], []
    for k in range(STEPS):
        norm = (weight * now * now).sum()
        centre = (weight * values * now * now).sum() / norm
        link = norm / norm_before if k else 0.0
        centres.append(float(centre))
        links.append(float(link))
        before, now, norm_before = now, (values - centre) * now - link * before, norm
    return float(scale), centres, links


SCALE, CENTRES, LINKS = recurrence()

BLOCKS = [(i, j) for i in range(4) for j in range(i, 4)]
SLOT = {}
for number, (bi, bj) in enumerate(BLOCKS):
    for a in range(4):
        for b in range(4):
            SLOT.setdefault((4 * bi + a, 4 * bj + b), number * 16 + a * 4 + b)


def lanes(shape):
    return lax.broadcasted_iota(jnp.int32, shape, 1)


def kernel(gy, *refs):
    ins, outs = refs[:5], refs[5:7]
    (buf, send, halo, plain, edge, speed, coef, field, image, acc, msg, every, spread, done, table,
     in_sem, part_sem, edge_sem, halo_sem, sum_sem, far_sem, meet) = refs[7:]
    c = lax.axis_index("gx")
    g = lax.axis_index("gy")
    n = 2 * gy
    me = c * gy + g
    mine = pl.multiple_of(c * 64, 64)
    theirs = pl.multiple_of((1 - c) * 64, 64)
    my_cols = pl.multiple_of(c * 128, 128)

    loads = [pltpu.make_async_copy(ins[q], buf.at[q, pl.ds(mine, 64)], in_sem.at[q]) for q in range(5)]
    for load in loads:
        load.start()

    sizes = (4, 4, 4) if gy == 64 else (1, 2, gy // 2)
    strides = (sizes[1] * sizes[2], sizes[2], 1)
    around = [
        [lax.rem(lax.rem(g // stride, size) + k, size) * stride for k in range(size)]
        for stride, size in zip(strides, sizes)
    ]
    ahead, behind = lax.rem(g + 1, gy), lax.rem(g + gy - 1, gy)

    def line(d):
        rest = g - around[d][0]
        return [(c, rest + around[d][k]) for k in sorted(range(1, sizes[d]), key=lambda k: k != sizes[d] // 2)]

    def signal(sem, to):
        pl.semaphore_signal(sem, inc=1, device_id=to, device_id_type=MESH)

    barrier = pltpu.get_barrier_semaphore()
    sender = jnp.where(c == 0, behind, ahead)
    across = [(1 - c, chip) for _, chip in line(0)]
    greeted = [(0, sender), (1, sender)] + line(0) + across + line(1) + line(2) + [(1 - c, g)]
    for to in greeted:
        signal(barrier, to)

    for k in range(STEPS):
        table[0, k] = CENTRES[k]
        table[1, k] = LINKS[k]
    for load in loads:
        load.wait()

    lane64 = lanes((64, 128))
    lane16 = lanes((16, 128))
    for way in range(2):
        tile, first = (1, 96) if way == 0 else (0, 0)
        packed = None
        for q in range(4):
            at = 32 * (q if way == 0 else (q + 1) % 4)
            piece = buf[q, pl.ds(mine, 64), pl.ds(128 * tile, 128)]
            shift = (at - first) % 128
            piece = pltpu.roll(piece, shift, 1) if shift else piece
            packed = piece if packed is None else jnp.where((lane64 >= at) & (lane64 < at + 32), piece, packed)
        send[way, pl.ds(0, 64)] = packed
        packed = None
        for q in range(4):
            at = 32 * (q if way == 0 else (q + 1) % 4)
            piece = buf[4, pl.ds(pl.multiple_of(mine + 16 * q, 16), 16), pl.ds(128 * tile, 128)]
            shift = (at - first) % 128
            piece = pltpu.roll(piece, shift, 1) if shift else piece
            packed = piece if packed is None else jnp.where((lane16 >= at) & (lane16 < at + 32), piece, packed)
        send[way, pl.ds(64, 16)] = packed

    pl.semaphore_wait(barrier, len(greeted))

    edges = []
    for way, (core, chip) in enumerate(((0, ahead), (1, behind))):
        copy = pltpu.make_async_remote_copy(
            send.at[way], halo.at[c], edge_sem.at[way], halo_sem.at[c], device_id=(core, chip), device_id_type=MESH
        )
        copy.start()
        edges.append(copy)
    part = pltpu.make_async_remote_copy(
        buf.at[:, pl.ds(mine, 64)], buf.at[:, pl.ds(mine, 64)], part_sem.at[0], part_sem.at[1],
        device_id=(1 - c, g), device_id_type=MESH,
    )
    part.start()
    for to in line(2):
        signal(meet.at[0], to)
    lane = lanes((CHUNK, 128))
    ROWS = range(0, 128, CHUNK)
    near = pl.multiple_of(128 - my_cols, 128)

    def turn_in(first):
        for q in range(5):
            for rows in range(0, 64, CHUNK):
                here = pl.ds(pl.multiple_of(first + rows, CHUNK), CHUNK)
                plain[q, here] = pltpu.roll(buf[q, here, pl.ds(my_cols, 128)], 32, 1)
                edge[q, here] = pltpu.roll(buf[q, here, pl.ds(near, 128)], 32, 1)

    turn_in(mine)
    part.wait_recv()
    turn_in(theirs)

    def put(ref, at, rows, value):
        ref[at + (pl.ds(8 + rows, CHUNK),)] = value
        if rows == 0:
            ref[at + (pl.ds(136, 8),)] = value[:8]
        if rows == 128 - CHUNK:
            ref[at + (pl.ds(0, 8),)] = value[CHUNK - 8 :]

    def operate(slot, tile, rows, centre):
        here = pl.ds(rows, CHUNK)
        turned = [
            coef[5 + number, here] * pltpu.roll(centre, (-offset) % 128, 1)
            for number, (offset, _, _) in enumerate(STENCIL)
        ]
        moved = [
            coef[1 + number, here] * field[slot, tile, pl.ds(8 + rows + offset, CHUNK)]
            for number, (offset, _, _) in enumerate(STENCIL)
        ]
        still = coef[0, here] * centre + ((moved[0] + moved[1]) + (moved[2] + moved[3]))
        return still, (turned[0] + turned[1]) + (turned[2] + turned[3])

    def half(phase, carry):
        tile = lax.rem(1 - c + phase, 2)

        @pl.when(phase == 1)
        def _():
            for side in range(2):
                pltpu.make_async_copy(halo.at[side], halo.at[side], halo_sem.at[side]).wait()
            for side in range(2):
                for q in range(4):
                    far = halo[side, pl.ds(0, 64)]
                    edge[q, pl.ds(64 * side, 64)] = pltpu.roll(far, 128 - 32 * q, 1) if q else far
                for q in range(4):
                    far = halo[side, pl.ds(64, 16)]
                    edge[4, pl.ds(64 * side + 16 * q, 16)] = pltpu.roll(far, 128 - 32 * q, 1) if q else far

        halo_lanes = (lane >= 32 * tile) & (lane < 32 * tile + 32)
        core_lanes = ((lane >= 32) & (lane < 96)).astype(jnp.int32) == 1 - tile

        def gather(q, rows):
            here = pl.ds(rows, CHUNK)
            return jnp.where(halo_lanes, edge[q, here], plain[q, here])

        for rows in ROWS:
            put(field, (0, tile), rows, gather(1, rows))
            put(speed, (), rows, gather(3, rows))
        for rows in ROWS:
            here = pl.ds(rows, CHUNK)
            coef[0, here] = SCALE * (gather(2, rows) + 5.0)
            vx = speed[pl.ds(8 + rows, CHUNK)]
            for number, (offset, flat, slope) in enumerate(STENCIL):
                other = speed[pl.ds(8 + rows + offset, CHUNK)]
                coef[1 + number, here] = flat + slope * (vx + other)
            vy = gather(4, rows)
            for number, (offset, flat, slope) in enumerate(STENCIL):
                other = pltpu.roll(vy, (-offset) % 128, 1)
                coef[5 + number, here] = flat + slope * (vy + other)
        for rows in ROWS:
            still, turned = operate(0, tile, rows, field[0, tile, pl.ds(8 + rows, CHUNK)])
            value = gather(0, rows) - (1.0 / SCALE) * (still + turned)
            put(field, (1, tile), rows, value)
            pltpu.store(image.at[STEPS, pl.ds(rows, CHUNK)], value, mask=core_lanes)

        def steps(turn, carry):
            centres = None
            for k in [turn * 5 + part for part in range(5)]:
                centre_k = table[0, k]
                link_k = table[1, k]
                afters = []
                for index, rows in enumerate(ROWS):
                    now = centres[index] if centres else field[k + 1, tile, pl.ds(8 + rows, CHUNK)]
                    still, turned = operate(k + 1, tile, rows, now)
                    before = field[k, tile, pl.ds(8 + rows, CHUNK)]
                    rest = still - centre_k * now - link_k * before
                    after = rest + turned
                    put(field, (k + 2, tile), rows, after)
                    pltpu.store(image.at[k, pl.ds(rows, CHUNK)], still + turned, mask=core_lanes)
                    afters.append(after)
                centres = afters
            return carry

        return lax.fori_loop(0, STEPS // 5, steps, carry)

    lax.fori_loop(0, 1, half, 0)
    pl.semaphore_wait(meet.at[0], sizes[2] - 1)
    for to in line(1):
        signal(meet.at[1], to)
    lax.fori_loop(1, 2, half, 0)

    def core(lane, first, second):
        return jnp.where((lane >= 32) & (lane < 96), first, second)

    for number, (bi, bj) in enumerate(BLOCKS):

        def products(row, sums, bi=bi, bj=bj):
            for part in range(8):
                at = pl.ds(pl.multiple_of(row * 64 + 8 * part, 8), 8)
                left = [image[4 * bi + a, at] for a in range(4)]
                right = left if bi == bj else [image[4 * bj + b, at] for b in range(4)]
                sums = tuple(
                    sums[4 * a + b] if bi == bj and a > b else sums[4 * a + b] + left[a] * right[b]
                    for a in range(4)
                    for b in range(4)
                )
            return sums

        sums = lax.fori_loop(0, 2, products, (jnp.zeros((8, 128), F32),) * 16)
        for a in range(16):
            acc[pl.ds(number * 128 + 8 * a, 8)] = sums[a]

    folded = [acc[pl.ds(part, 160, stride=8)] for part in range(8)]
    while len(folded) > 1:
        folded = [one + other for one, other in zip(folded[::2], folded[1::2])]
    totals = jnp.sum(folded[0], axis=1, keepdims=True)
    wide = jnp.broadcast_to(totals[:128], (128, 128))
    pick = lax.broadcasted_iota(jnp.int32, (128, 128), 0) == lanes((128, 128))
    msg[pl.ds(0, 1)] = jnp.sum(jnp.where(pick, wide, 0.0), axis=0, keepdims=True)
    wide = jnp.broadcast_to(totals[128:], (32, 128))
    msg[pl.ds(1, 1)] = jnp.sum(jnp.where(pick[:32], wide, 0.0), axis=0, keepdims=True)

    pl.semaphore_wait(meet.at[1], sizes[1] - 1)

    def hops(way):
        return sum(min(k, size - k) for k, size in zip(way[:3], sizes)) + 0.5 * way[3]

    ways = [(z, y, x, w) for z in range(sizes[0]) for y in range(sizes[1]) for x in range(sizes[2]) for w in range(2)]
    for z, y, x, w in sorted(ways[1:], key=hops, reverse=True):
        pltpu.make_async_remote_copy(
            msg, every.at[me], sum_sem.at[0], sum_sem.at[1],
            device_id=(1 - c if w else c, around[0][z] + around[1][y] + around[2][x]), device_id_type=MESH,
        ).start()
    every[me] = msg[...]
    others = every.at[pl.ds(0, n - 1)]
    pltpu.make_async_copy(others, others, sum_sem.at[1]).wait()
    width = n // 2
    total = every[pl.ds(0, width)] + every[pl.ds(width, width)]
    while width > 1:
        width //= 2
        total = total[:width] + total[width:]
    total = total[0]

    wide = jnp.where(pick, jnp.broadcast_to(total[0:1], (128, 128)), 0.0)
    spread[pl.ds(0, 128)] = jnp.broadcast_to(jnp.sum(wide, axis=1, keepdims=True), (128, 128))
    wide = jnp.where(pick[:32], jnp.broadcast_to(total[1:2], (32, 128)), 0.0)
    spread[pl.ds(128, 32)] = jnp.broadcast_to(jnp.sum(wide, axis=1, keepdims=True), (32, 128))

    def entry(i, j):
        at = SLOT[(min(i, j), max(i, j))]
        return jnp.broadcast_to(spread[at : at + 1], (8, 128))

    gram = [[entry(i, j) for j in range(i + 1)] for i in range(STEPS)]
    goal = [entry(i, STEPS) for i in range(STEPS)]
    inverse = []
    for k in range(STEPS):
        inverse.append(1.0 / gram[k][k])
        for i in range(k + 1, STEPS):
            ratio = gram[i][k] * inverse[k]
            for j in range(k + 1, i + 1):
                gram[i][j] = gram[i][j] - ratio * gram[j][k]
            goal[i] = goal[i] - ratio * goal[k]
    weights = [None] * STEPS
    for k in reversed(range(STEPS)):
        value = goal[k]
        for i in range(k + 1, STEPS):
            value = value - gram[i][k] * weights[i]
        weights[k] = value * inverse[k]

    lane8 = lanes((8, 128))
    inside = (lane8 >= 32) & (lane8 < 96)

    def finish(first):
        def some(row, carry):
            for part in range(4):
                at = pl.ds(pl.multiple_of(first + row * 32 + 8 * part, 8), 8)
                inner = pl.ds(pl.multiple_of(first + row * 32 + 8 * part + 8, 8), 8)
                leftover = image[STEPS, at]
                change = None
                for k in range(STEPS):
                    leftover = leftover - weights[k] * image[k, at]
                    term = weights[k] * jnp.where(inside, field[k + 1, 0, inner], field[k + 1, 1, inner])
                    change = term if change is None else change + term
                start = jnp.where(inside, field[0, 0, inner], field[0, 1, inner])
                done[0, at] = pltpu.roll(start + SCALE * change, 96, 1)
                done[1, at] = pltpu.roll(leftover, 96, 1)
            return carry

        lax.fori_loop(0, 2, some, 0)

    finish(theirs)
    aways = []
    for o in range(2):
        away = pltpu.make_async_remote_copy(
            done.at[o, pl.ds(theirs, 64)], outs[o].at[:, pl.ds(my_cols, 128)], far_sem.at[0, o], far_sem.at[1, o],
            device_id=(1 - c, g), device_id_type=MESH,
        )
        away.start()
        aways.append(away)
    finish(mine)
    for o in range(2):
        outs[o][:, pl.ds(my_cols, 128)] = done[o, pl.ds(mine, 64)]
    for away in aways:
        away.wait()
    part.wait_send()
    for edge_copy in edges:
        edge_copy.wait_send()
    pltpu.make_async_copy(others, others, sum_sem.at[0]).wait()


STENCIL = [
    (-2, SCALE / 12.0, SCALE / 24.0),
    (-1, -SCALE * 16.0 / 12.0, -SCALE * 8.0 / 24.0),
    (1, -SCALE * 16.0 / 12.0, SCALE * 8.0 / 24.0),
    (2, SCALE / 12.0, -SCALE / 24.0),
]


def write(*refs):
    moves = [pltpu.make_async_copy(refs[o], refs[2 + o], refs[4].at[o]) for o in range(2)]
    for move in moves:
        move.start()
    for move in moves:
        move.wait()


def solution(mesh):
    gy = mesh.shape["gy"]
    n = 2 * gy
    anywhere = pl.BlockSpec(memory_space=pl.ANY)

    def per_device(*blocks):
        blocks = [pltpu.with_memory_space_constraint(block, pltpu.HBM) for block in blocks]
        both = pl.pallas_call(
            functools.partial(kernel, gy),
            out_shape=[jax.ShapeDtypeStruct((64, 256), F32)] * 2,
            in_specs=[anywhere] * 5,
            out_specs=[pl.BlockSpec(memory_space=pltpu.VMEM)] * 2,
            scratch_shapes=[
                pltpu.VMEM((5, 128, 256), F32),
                pltpu.VMEM((2, 80, 128), F32),
                pltpu.VMEM((2, 80, 128), F32),
                pltpu.VMEM((5, 128, 128), F32),
                pltpu.VMEM((5, 128, 128), F32),
                pltpu.VMEM((144, 128), F32),
                pltpu.VMEM((9, 128, 128), F32),
                pltpu.VMEM((STEPS + 2, 2, 144, 128), F32),
                pltpu.VMEM((STEPS + 1, 128, 128), F32),
                pltpu.VMEM((1280, 128), F32),
                pltpu.VMEM((2, 128), F32),
                pltpu.VMEM((n, 2, 128), F32),
                pltpu.VMEM((160, 128), F32),
                pltpu.VMEM((2, 128, 128), F32),
                pltpu.SMEM((2, 16), F32),
                pltpu.SemaphoreType.DMA((5,)),
                pltpu.SemaphoreType.DMA((2,)),
                pltpu.SemaphoreType.DMA((2,)),
                pltpu.SemaphoreType.DMA((2,)),
                pltpu.SemaphoreType.DMA((2,)),
                pltpu.SemaphoreType.DMA((2, 2)),
                pltpu.SemaphoreType.REGULAR((2,)),
            ],
            compiler_params=pltpu.CompilerParams(collective_id=0, has_side_effects=True, vmem_limit_bytes=12 << 20),
        )(*blocks)
        return pl.pallas_call(
            write,
            out_shape=[jax.ShapeDtypeStruct((64, 256), F32)] * 2,
            in_specs=[anywhere] * 2,
            out_specs=[anywhere] * 2,
            scratch_shapes=[pltpu.SemaphoreType.DMA((2,))],
        )(*[pltpu.with_memory_space_constraint(one, pltpu.VMEM) for one in both])

    placed = P("gx", "gy")
    return jax.shard_map(
        per_device, mesh=mesh, in_specs=(placed,) * 5, out_specs=(placed, placed), check_vma=False
    )
```

```python
import functools

import jax
import jax.numpy as jnp
import numpy as np
from jax import lax
from jax.experimental import pallas as pl
from jax.experimental.pallas import tpu as pltpu
from jax.sharding import PartitionSpec as P

MESH = pl.DeviceIdType.MESH
STEPS = 15
CHUNK = 32
F32 = jnp.float32


def recurrence():
    count = 128
    angle = (np.arange(count) + 0.5) * np.pi / count
    one = (30.0 - 32.0 * np.cos(angle) + 2.0 * np.cos(2.0 * angle)) / 12.0
    values = (0.2 + one[:, None] + one[None, :]).ravel()
    weight = values * values
    scale = 4.0 / (values.max() - values.min())
    values = values * scale
    before, now, norm_before = np.zeros_like(values), np.ones_like(values), 1.0
    centres, links = [], []
    for k in range(STEPS):
        norm = (weight * now * now).sum()
        centre = (weight * values * now * now).sum() / norm
        link = norm / norm_before if k else 0.0
        centres.append(float(centre))
        links.append(float(link))
        before, now, norm_before = now, (values - centre) * now - link * before, norm
    return float(scale), centres, links


SCALE, CENTRES, LINKS = recurrence()

BLOCKS = [(i, j) for i in range(4) for j in range(i, 4)]
SLOT = {}
for number, (bi, bj) in enumerate(BLOCKS):
    for a in range(4):
        for b in range(4):
            SLOT.setdefault((4 * bi + a, 4 * bj + b), number * 16 + a * 4 + b)


def lanes(shape):
    return lax.broadcasted_iota(jnp.int32, shape, 1)


def kernel(gy, *refs):
    ins, outs = refs[:5], refs[5:7]
    (buf, send, halo, plain, edge, speed, coef, field, image, acc, msg, every, spread, done, table,
     in_sem, part_sem, edge_sem, halo_sem, sum_sem, far_sem, meet) = refs[7:]
    c = lax.axis_index("gx")
    g = lax.axis_index("gy")
    n = 2 * gy
    me = c * gy + g
    mine = pl.multiple_of(c * 64, 64)
    theirs = pl.multiple_of((1 - c) * 64, 64)
    my_cols = pl.multiple_of(c * 128, 128)

    loads = [pltpu.make_async_copy(ins[q], buf.at[q, pl.ds(mine, 64)], in_sem.at[q]) for q in range(5)]
    for load in loads:
        load.start()

    sizes = (4, 4, 4) if gy == 64 else (1, 2, gy // 2)
    strides = (sizes[1] * sizes[2], sizes[2], 1)
    around = [
        [lax.rem(lax.rem(g // stride, size) + k, size) * stride for k in range(size)]
        for stride, size in zip(strides, sizes)
    ]
    ahead, behind = lax.rem(g + 1, gy), lax.rem(g + gy - 1, gy)

    def line(d):
        rest = g - around[d][0]
        return [(c, rest + around[d][k]) for k in sorted(range(1, sizes[d]), key=lambda k: k != sizes[d] // 2)]

    def signal(sem, to):
        pl.semaphore_signal(sem, inc=1, device_id=to, device_id_type=MESH)

    barrier = pltpu.get_barrier_semaphore()
    sender = jnp.where(c == 0, behind, ahead)
    across = [(1 - c, chip) for _, chip in line(0)]
    greeted = [(0, sender), (1, sender)] + line(0) + across + line(1) + line(2) + [(1 - c, g)]
    for to in greeted:
        signal(barrier, to)

    for k in range(STEPS):
        table[0, k] = CENTRES[k]
        table[1, k] = LINKS[k]
    for load in loads:
        load.wait()

    lane64 = lanes((64, 128))
    lane16 = lanes((16, 128))
    for way in range(2):
        tile, first = (1, 96) if way == 0 else (0, 0)
        packed = None
        for q in range(4):
            at = 32 * (q if way == 0 else (q + 1) % 4)
            piece = buf[q, pl.ds(mine, 64), pl.ds(128 * tile, 128)]
            shift = (at - first) % 128
            piece = pltpu.roll(piece, shift, 1) if shift else piece
            packed = piece if packed is None else jnp.where((lane64 >= at) & (lane64 < at + 32), piece, packed)
        send[way, pl.ds(0, 64)] = packed
        packed = None
        for q in range(4):
            at = 32 * (q if way == 0 else (q + 1) % 4)
            piece = buf[4, pl.ds(pl.multiple_of(mine + 16 * q, 16), 16), pl.ds(128 * tile, 128)]
            shift = (at - first) % 128
            piece = pltpu.roll(piece, shift, 1) if shift else piece
            packed = piece if packed is None else jnp.where((lane16 >= at) & (lane16 < at + 32), piece, packed)
        send[way, pl.ds(64, 16)] = packed

    pl.semaphore_wait(barrier, len(greeted))

    edges = []
    for way, (core, chip) in enumerate(((0, ahead), (1, behind))):
        copy = pltpu.make_async_remote_copy(
            send.at[way], halo.at[c], edge_sem.at[way], halo_sem.at[c], device_id=(core, chip), device_id_type=MESH
        )
        copy.start()
        edges.append(copy)
    part = pltpu.make_async_remote_copy(
        buf.at[:, pl.ds(mine, 64)], buf.at[:, pl.ds(mine, 64)], part_sem.at[0], part_sem.at[1],
        device_id=(1 - c, g), device_id_type=MESH,
    )
    part.start()
    for to in line(2):
        signal(meet.at[0], to)
    lane = lanes((CHUNK, 128))
    ROWS = range(0, 128, CHUNK)
    near = pl.multiple_of(128 - my_cols, 128)

    def turn_in(first):
        for q in range(5):
            for rows in range(0, 64, CHUNK):
                here = pl.ds(pl.multiple_of(first + rows, CHUNK), CHUNK)
                plain[q, here] = pltpu.roll(buf[q, here, pl.ds(my_cols, 128)], 32, 1)
                edge[q, here] = pltpu.roll(buf[q, here, pl.ds(near, 128)], 32, 1)

    turn_in(mine)
    part.wait_recv()
    turn_in(theirs)

    def put(ref, at, rows, value):
        ref[at + (pl.ds(8 + rows, CHUNK),)] = value
        if rows == 0:
            ref[at + (pl.ds(136, 8),)] = value[:8]
        if rows == 128 - CHUNK:
            ref[at + (pl.ds(0, 8),)] = value[CHUNK - 8 :]

    def operate(slot, tile, rows, centre):
        here = pl.ds(rows, CHUNK)
        turned = [
            coef[5 + number, here] * pltpu.roll(centre, (-offset) % 128, 1)
            for number, (offset, _, _) in enumerate(STENCIL)
        ]
        moved = [
            coef[1 + number, here] * field[slot, tile, pl.ds(8 + rows + offset, CHUNK)]
            for number, (offset, _, _) in enumerate(STENCIL)
        ]
        still = coef[0, here] * centre + ((moved[0] + moved[1]) + (moved[2] + moved[3]))
        return still, (turned[0] + turned[1]) + (turned[2] + turned[3])

    def half(phase, carry):
        tile = lax.rem(1 - c + phase, 2)

        @pl.when(phase == 1)
        def _():
            for side in range(2):
                pltpu.make_async_copy(halo.at[side], halo.at[side], halo_sem.at[side]).wait()
            for side in range(2):
                for q in range(4):
                    far = halo[side, pl.ds(0, 64)]
                    edge[q, pl.ds(64 * side, 64)] = pltpu.roll(far, 128 - 32 * q, 1) if q else far
                for q in range(4):
                    far = halo[side, pl.ds(64, 16)]
                    edge[4, pl.ds(64 * side + 16 * q, 16)] = pltpu.roll(far, 128 - 32 * q, 1) if q else far

        halo_lanes = (lane >= 32 * tile) & (lane < 32 * tile + 32)
        core_lanes = ((lane >= 32) & (lane < 96)).astype(jnp.int32) == 1 - tile

        def gather(q, rows):
            here = pl.ds(rows, CHUNK)
            return jnp.where(halo_lanes, edge[q, here], plain[q, here])

        for rows in ROWS:
            put(field, (0, tile), rows, gather(1, rows))
            put(speed, (), rows, gather(3, rows))
        for rows in ROWS:
            here = pl.ds(rows, CHUNK)
            coef[0, here] = SCALE * (gather(2, rows) + 5.0)
            vx = speed[pl.ds(8 + rows, CHUNK)]
            for number, (offset, flat, slope) in enumerate(STENCIL):
                other = speed[pl.ds(8 + rows + offset, CHUNK)]
                coef[1 + number, here] = flat + slope * (vx + other)
            vy = gather(4, rows)
            for number, (offset, flat, slope) in enumerate(STENCIL):
                other = pltpu.roll(vy, (-offset) % 128, 1)
                coef[5 + number, here] = flat + slope * (vy + other)
        for rows in ROWS:
            still, turned = operate(0, tile, rows, field[0, tile, pl.ds(8 + rows, CHUNK)])
            value = gather(0, rows) - (1.0 / SCALE) * (still + turned)
            put(field, (1, tile), rows, value)
            pltpu.store(image.at[STEPS, pl.ds(rows, CHUNK)], value, mask=core_lanes)

        def steps(turn, carry):
            centres = None
            for k in [turn * 5 + part for part in range(5)]:
                centre_k = table[0, k]
                link_k = table[1, k]
                afters = []
                for index, rows in enumerate(ROWS):
                    now = centres[index] if centres else field[k + 1, tile, pl.ds(8 + rows, CHUNK)]
                    still, turned = operate(k + 1, tile, rows, now)
                    before = field[k, tile, pl.ds(8 + rows, CHUNK)]
                    rest = still - centre_k * now - link_k * before
                    after = rest + turned
                    put(field, (k + 2, tile), rows, after)
                    pltpu.store(image.at[k, pl.ds(rows, CHUNK)], still + turned, mask=core_lanes)
                    afters.append(after)
                centres = afters
            return carry

        return lax.fori_loop(0, STEPS // 5, steps, carry)

    lax.fori_loop(0, 1, half, 0)
    pl.semaphore_wait(meet.at[0], sizes[2] - 1)
    for to in line(1):
        signal(meet.at[1], to)
    lax.fori_loop(1, 2, half, 0)

    def core(lane, first, second):
        return jnp.where((lane >= 32) & (lane < 96), first, second)

    for number, (bi, bj) in enumerate(BLOCKS):

        def products(row, sums, bi=bi, bj=bj):
            for part in range(8):
                at = pl.ds(pl.multiple_of(row * 64 + 8 * part, 8), 8)
                left = [image[4 * bi + a, at] for a in range(4)]
                right = left if bi == bj else [image[4 * bj + b, at] for b in range(4)]
                sums = tuple(
                    sums[4 * a + b] if bi == bj and a > b else sums[4 * a + b] + left[a] * right[b]
                    for a in range(4)
                    for b in range(4)
                )
            return sums

        sums = lax.fori_loop(0, 2, products, (jnp.zeros((8, 128), F32),) * 16)
        for a in range(16):
            acc[pl.ds(number * 128 + 8 * a, 8)] = sums[a]

    folded = [acc[pl.ds(part, 160, stride=8)] for part in range(8)]
    while len(folded) > 1:
        folded = [one + other for one, other in zip(folded[::2], folded[1::2])]
    totals = jnp.sum(folded[0], axis=1, keepdims=True)
    wide = jnp.broadcast_to(totals[:128], (128, 128))
    pick = lax.broadcasted_iota(jnp.int32, (128, 128), 0) == lanes((128, 128))
    msg[pl.ds(0, 1)] = jnp.sum(jnp.where(pick, wide, 0.0), axis=0, keepdims=True)
    wide = jnp.broadcast_to(totals[128:], (32, 128))
    msg[pl.ds(1, 1)] = jnp.sum(jnp.where(pick[:32], wide, 0.0), axis=0, keepdims=True)

    pl.semaphore_wait(meet.at[1], sizes[1] - 1)

    def hops(way):
        return sum(min(k, size - k) for k, size in zip(way[:3], sizes)) + 0.5 * way[3]

    ways = [(z, y, x, w) for z in range(sizes[0]) for y in range(sizes[1]) for x in range(sizes[2]) for w in range(2)]
    for z, y, x, w in sorted(ways[1:], key=hops, reverse=True):
        pltpu.make_async_remote_copy(
            msg, every.at[me], sum_sem.at[0], sum_sem.at[1],
            device_id=(1 - c if w else c, around[0][z] + around[1][y] + around[2][x]), device_id_type=MESH,
        ).start()
    every[me] = msg[...]
    others = every.at[pl.ds(0, n - 1)]
    pltpu.make_async_copy(others, others, sum_sem.at[1]).wait()
    width = n // 2
    total = every[pl.ds(0, width)] + every[pl.ds(width, width)]
    while width > 1:
        width //= 2
        total = total[:width] + total[width:]
    total = total[0]

    wide = jnp.where(pick, jnp.broadcast_to(total[0:1], (128, 128)), 0.0)
    spread[pl.ds(0, 128)] = jnp.broadcast_to(jnp.sum(wide, axis=1, keepdims=True), (128, 128))
    wide = jnp.where(pick[:32], jnp.broadcast_to(total[1:2], (32, 128)), 0.0)
    spread[pl.ds(128, 32)] = jnp.broadcast_to(jnp.sum(wide, axis=1, keepdims=True), (32, 128))

    def entry(i, j):
        at = SLOT[(min(i, j), max(i, j))]
        return jnp.broadcast_to(spread[at : at + 1], (8, 128))

    gram = [[entry(i, j) for j in range(i + 1)] for i in range(STEPS)]
    goal = [entry(i, STEPS) for i in range(STEPS)]
    inverse = []
    for k in range(STEPS):
        inverse.append(1.0 / gram[k][k])
        for i in range(k + 1, STEPS):
            ratio = gram[i][k] * inverse[k]
            for j in range(k + 1, i + 1):
                gram[i][j] = gram[i][j] - ratio * gram[j][k]
            goal[i] = goal[i] - ratio * goal[k]
    weights = [None] * STEPS
    for k in reversed(range(STEPS)):
        value = goal[k]
        for i in reversed(range(k + 1, STEPS)):
            value = value - gram[i][k] * weights[i]
        weights[k] = value * inverse[k]

    lane8 = lanes((8, 128))
    inside = (lane8 >= 32) & (lane8 < 96)

    def finish(first):
        def some(row, carry):
            for part in range(4):
                at = pl.ds(pl.multiple_of(first + row * 32 + 8 * part, 8), 8)
                inner = pl.ds(pl.multiple_of(first + row * 32 + 8 * part + 8, 8), 8)
                leftover = image[STEPS, at]
                change = None
                for k in range(STEPS):
                    leftover = leftover - weights[k] * image[k, at]
                    term = weights[k] * jnp.where(inside, field[k + 1, 0, inner], field[k + 1, 1, inner])
                    change = term if change is None else change + term
                start = jnp.where(inside, field[0, 0, inner], field[0, 1, inner])
                done[0, at] = pltpu.roll(start + SCALE * change, 96, 1)
                done[1, at] = pltpu.roll(leftover, 96, 1)
            return carry

        lax.fori_loop(0, 2, some, 0)

    finish(theirs)
    aways = []
    for o in range(2):
        away = pltpu.make_async_remote_copy(
            done.at[o, pl.ds(theirs, 64)], outs[o].at[:, pl.ds(my_cols, 128)], far_sem.at[0, o], far_sem.at[1, o],
            device_id=(1 - c, g), device_id_type=MESH,
        )
        away.start()
        aways.append(away)
    finish(mine)
    for o in range(2):
        outs[o][:, pl.ds(my_cols, 128)] = done[o, pl.ds(mine, 64)]
    for away in aways:
        away.wait()
    part.wait_send()
    for edge_copy in edges:
        edge_copy.wait_send()
    pltpu.make_async_copy(others, others, sum_sem.at[0]).wait()


STENCIL = [
    (-2, SCALE / 12.0, SCALE / 24.0),
    (-1, -SCALE * 16.0 / 12.0, -SCALE * 8.0 / 24.0),
    (1, -SCALE * 16.0 / 12.0, SCALE * 8.0 / 24.0),
    (2, SCALE / 12.0, -SCALE / 24.0),
]


def write(*refs):
    moves = [pltpu.make_async_copy(refs[o], refs[2 + o], refs[4].at[o]) for o in range(2)]
    for move in moves:
        move.start()
    for move in moves:
        move.wait()


def solution(mesh):
    gy = mesh.shape["gy"]
    n = 2 * gy
    anywhere = pl.BlockSpec(memory_space=pl.ANY)

    def per_device(*blocks):
        blocks = [pltpu.with_memory_space_constraint(block, pltpu.HBM) for block in blocks]
        both = pl.pallas_call(
            functools.partial(kernel, gy),
            out_shape=[jax.ShapeDtypeStruct((64, 256), F32)] * 2,
            in_specs=[anywhere] * 5,
            out_specs=[pl.BlockSpec(memory_space=pltpu.VMEM)] * 2,
            scratch_shapes=[
                pltpu.VMEM((5, 128, 256), F32),
                pltpu.VMEM((2, 80, 128), F32),
                pltpu.VMEM((2, 80, 128), F32),
                pltpu.VMEM((5, 128, 128), F32),
                pltpu.VMEM((5, 128, 128), F32),
                pltpu.VMEM((144, 128), F32),
                pltpu.VMEM((9, 128, 128), F32),
                pltpu.VMEM((STEPS + 2, 2, 144, 128), F32),
                pltpu.VMEM((STEPS + 1, 128, 128), F32),
                pltpu.VMEM((1280, 128), F32),
                pltpu.VMEM((2, 128), F32),
                pltpu.VMEM((n, 2, 128), F32),
                pltpu.VMEM((160, 128), F32),
                pltpu.VMEM((2, 128, 128), F32),
                pltpu.SMEM((2, 16), F32),
                pltpu.SemaphoreType.DMA((5,)),
                pltpu.SemaphoreType.DMA((2,)),
                pltpu.SemaphoreType.DMA((2,)),
                pltpu.SemaphoreType.DMA((2,)),
                pltpu.SemaphoreType.DMA((2,)),
                pltpu.SemaphoreType.DMA((2, 2)),
                pltpu.SemaphoreType.REGULAR((2,)),
            ],
            compiler_params=pltpu.CompilerParams(collective_id=0, has_side_effects=True, vmem_limit_bytes=12 << 20),
        )(*blocks)
        return pl.pallas_call(
            write,
            out_shape=[jax.ShapeDtypeStruct((64, 256), F32)] * 2,
            in_specs=[anywhere] * 2,
            out_specs=[anywhere] * 2,
            scratch_shapes=[pltpu.SemaphoreType.DMA((2,))],
        )(*[pltpu.with_memory_space_constraint(one, pltpu.VMEM) for one in both])

    placed = P("gx", "gy")
    return jax.shard_map(
        per_device, mesh=mesh, in_specs=(placed,) * 5, out_specs=(placed, placed), check_vma=False
    )
```
